32 devices in a mesh: panel: 8 (over z, y), obs: 4 (over x, core).
Axes of the slice: x: 2, y: 2, z: 4, core: 2. Of those that a mesh axis runs over, the one named last changes fastest.
Arguments:
- flow_blocks: bfloat16 [1024, 4, 1280], P('panel'), may hold values from -6 to 6
- interp_weights: bfloat16 [32, 128, 512], P(('panel', 'obs')), may hold values from -0.25 to 0.25
- donor_owner: int32 [4096, 1], P(('panel', 'obs')), may hold values from 0 to 7; in each aligned block of 128 rows (0 to 127, 128 to 255, ...) at most 24 rows name the same one
- donor_block: int32 [4096], P(('panel', 'obs')), may hold values from 0 to 127
- panel_normals: float32 [3, 4096], P(None, ('panel', 'obs')), may hold values from -3 to 3
- panel_points: float32 [3, 4096], P(None, ('panel', 'obs')), may hold values from -1 to 1
- observer_points: float32 [3, 1024], P(None, 'obs'), may hold values from -12 to 12, as said below
Outputs:
- pressure: float32 [128, 1024], P('panel', 'obs')
The draws below stay inside these ranges and needn't reach their ends.
Inputs may be any that keep to these rules, and one draw needn't show every extreme that they name: `donor_owner`: within the rows of one device, no owner index is named by more than 24 rows; some devices' rows name one owner exactly 24 times. `observer_points`: every observer lies between 6 and 12 from the anchor.
All inputs are finite; a program needn't handle non-finite values.
Results may differ from the reference program's by a relative error of at most 0.0003.
Values may be sent and summed in bfloat16 or wider, within the bound.
A program may use at most 64 MiB of HBM per device.

```python
import math
import jax
import jax.numpy as jnp
import numpy as np
from jax import lax

NV = 5
NT = 256
HARM = 64
TILE = 128
SLOTS = 128
CB = 4
GB_DEV = 128
TILE_DEV = 1
TILES = 32
PANELS = 4096
BLOCKS = 1024
OBS = 1024
CAP = 24
N_PANEL = 8


def draw_observer_points(key, part):
    key_height, key_turn, key_radius = jax.random.split(key, 3)
    height = jax.random.uniform(key_height, (OBS,), jnp.float32, -1.0, 1.0)
    turn = jax.random.uniform(key_turn, (OBS,), jnp.float32, -math.pi, math.pi)
    radius = jax.random.uniform(key_radius, (OBS,), jnp.float32, 6.0, 12.0)
    side = jnp.sqrt(jnp.maximum(1.0 - height * height, 0.0))
    return jnp.stack([radius * side * jnp.cos(turn), radius * side * jnp.sin(turn), radius * height])


def plant(array, key, smallest, top_value):
    shape = array.shape
    spot = [jax.random.randint(jax.random.fold_in(key, axis), (), 0, shape[axis]) for axis in range(len(shape))]
    array = array.at[tuple(spot)].set(smallest)
    longest = shape.index(max(shape))
    spot[longest] = (spot[longest] + 1) % shape[longest]
    return array.at[tuple(spot)].set(top_value)


def level_of(stream_key, dims, cuts, least, high):
    gain = 1.0
    for axis_at, shards_of in cuts:
        heights = jax.random.uniform(jax.random.fold_in(jax.random.fold_in(stream_key, 6), axis_at), (shards_of,), jnp.float32, least / len(cuts), high / len(cuts))
        gain = gain * jnp.repeat(jnp.exp(heights), dims[axis_at] // shards_of).reshape((-1,) + (1,) * (len(dims) - 1 - axis_at))
    return gain


def assign_block(stream_key, own, number, rows, amount, top, limit, slope):
    sequence = jax.random.permutation(stream_key, amount)
    packed, ordinary = shares(amount, rows * top, limit, slope, True), shares(amount, rows * top, limit, slope, False)
    places = jnp.arange(amount)

    def named(tallies, turn):
        used = int((tallies > 0).sum())
        fixed = max(1, used // 4)
        moved = fixed + (places - fixed + turn * (used - fixed)) % max(1, amount - fixed)
        return jnp.zeros((amount,), jnp.int32).at[sequence[jnp.where(places < fixed, places, moved)]].set(jnp.asarray(tallies, jnp.int32))

    tallies = jnp.where(number % 4 == 0, named(packed, number // 4), named(ordinary, number - number // 4 - 1))
    mixed = jax.random.permutation(jax.random.fold_in(own, 3), amount)
    donor, sink = mixed[0:amount // 2 * 2:2], mixed[1:amount // 2 * 2:2]
    slack = jnp.minimum(tallies[donor] - 1, limit - tallies[sink]) // 2
    slack = jnp.where((donor == sequence[0]) | (sink == sequence[0]) | (tallies[sink] == 0), 0, jnp.maximum(slack, 0))
    moved = jax.random.randint(jax.random.fold_in(own, 4), (amount // 2,), 0, 1 << 20) % (slack + 1)
    tallies = tallies.at[donor].add(-moved).at[sink].add(moved)
    items = jnp.searchsorted(jnp.cumsum(tallies), jnp.arange(rows * top), side="right").astype(jnp.int32)
    table = items.reshape(top, rows).T
    table = table[jax.random.permutation(jax.random.fold_in(own, 1), rows)]
    turn = jax.random.randint(jax.random.fold_in(own, 2), (rows, 1), 0, top)
    return jnp.take_along_axis(table, (jnp.arange(top)[None, :] + turn) % top, axis=1)


def shares(number_of, total, most, lean, full):
    weights = [(1 << 20) // math.isqrt(standing ** lean) + 1 for standing in range(1, number_of + 1)]
    largest = most if full else min(most, max(-(-total // number_of), total * weights[0] // sum(weights)))
    least = 1 if total - largest >= number_of - 1 else 0
    holding, surplus = [largest] + [least] * (number_of - 1), total - largest - least * (number_of - 1)
    while surplus > 0:
        candidates = [i for i in range(1, number_of) if holding[i] < largest] or [i for i in range(1, number_of) if holding[i] < most]
        whole, left = sum([weights[i] for i in candidates]), surplus
        for i in candidates:
            addition = min(most - holding[i], max(1, left * weights[i] // whole), surplus)
            holding[i] = holding[i] + addition
            surplus = surplus - addition
    return np.array(holding)


def noise(stream_key, shape, width, limit, pieces=(), kind=jnp.bfloat16):
    entries = jax.random.normal(stream_key, shape, jnp.float32) * width
    if len(pieces) > 0:
        entries = level_of(stream_key, shape, pieces, -0.22, 0.18) * entries
    return jnp.clip(entries, min=-limit, max=limit).astype(kind)


def setup_inputs(seed: int = 0) -> dict:
    arg_keys = jax.random.split(jax.random.key(seed), 8)
    flow_blocks = noise(arg_keys[0], (BLOCKS, CB, NV * NT), 1.0, 6.0, ((0, 8),))
    interp_weights = noise(arg_keys[1], (TILES, TILE, SLOTS * CB), (SLOTS * CB) ** -0.5, 0.25, ((0, 32),))
    donor_owner_keys = jax.random.split(jax.random.fold_in(arg_keys[2], 1), (TILES * SLOTS) // (TILE_DEV * SLOTS))
    donor_owner_turns = jax.random.permutation(jax.random.fold_in(arg_keys[2], 3), (TILES * SLOTS) // (TILE_DEV * SLOTS))
    donor_owner = jax.vmap(lambda own, number: assign_block(jax.random.fold_in(arg_keys[2], 2), own, number, TILE_DEV * SLOTS, N_PANEL, 1, CAP, 2))(donor_owner_keys, donor_owner_turns).reshape((TILES * SLOTS, 1))
    donor_block = plant(jax.random.randint(arg_keys[3], (TILES * SLOTS,), 0, GB_DEV), jax.random.fold_in(arg_keys[3], 1), 0, GB_DEV - 1).astype(jnp.int32)
    panel_normals = noise(arg_keys[4], (3, PANELS), (30.0 * PANELS ** -0.5), 3.0, ((1, 32),), jnp.float32)
    panel_points = jnp.clip(jax.random.uniform(arg_keys[5], (3, PANELS), jnp.float32, -1.0, 1.0) * level_of(arg_keys[5], (3, PANELS), ((1, 32),), -0.4, 0.0), -1.0, 1.0)
    observer_points = draw_observer_points(jax.random.fold_in(arg_keys[7], 71), 0)
    return dict(flow_blocks=flow_blocks, interp_weights=interp_weights, donor_owner=donor_owner, donor_block=donor_block, panel_normals=panel_normals, panel_points=panel_points, observer_points=observer_points)


KAPPA = 0.5

def fourier_table(samples, orders):
    sample_ids = jnp.arange(samples, dtype=jnp.int32)
    harmonic = jnp.arange(1, orders + 1, dtype=jnp.int32)
    wrapped = sample_ids[:, None] * harmonic[None, :] % samples
    angles = wrapped.astype(jnp.float32) * (2.0 * math.pi / samples)
    factor = 2.0 / samples
    return jnp.concatenate([factor * jnp.cos(angles), -factor * jnp.sin(angles)], axis=1)

def spectra_of(values, normals, transform, samples):
    panels = values.shape[0]
    fields = values.reshape(panels, NV, samples)
    density = 1.0 + fields[:, 0]
    velocity = fields[:, 1:4]
    pressure_pert = fields[:, 4]
    normal_vec = jnp.transpose(normals)[:, :, None]
    normal_flow = lax.optimization_barrier(jnp.sum(velocity * normal_vec, axis=1))
    mass_flux = density * normal_flow
    loading = pressure_pert[:, None, :] * normal_vec + mass_flux[:, None, :] * velocity
    series = jnp.concatenate([mass_flux[:, None, :], loading], axis=1)
    return jnp.einsum('pct,tk->ckp', series, transform, precision=lax.Precision.HIGHEST)

def radiate(spectra, points, observers):
    orders = spectra.shape[1] // 2
    offset_vec = observers[:, None, :] - points[:, :, None]
    distance = jnp.sqrt(lax.optimization_barrier(jnp.sum(offset_vec * offset_vec, axis=0)))
    inverse = 1.0 / distance
    direction = offset_vec * inverse[None]
    wavenum = (KAPPA * jnp.arange(1, orders + 1, dtype=jnp.float32))[:, None, None]
    load_re = spectra[1, :orders][:, :, None] * direction[0][None] + spectra[2, :orders][:, :, None] * direction[1][None] + spectra[3, :orders][:, :, None] * direction[2][None]
    load_im = spectra[1, orders:][:, :, None] * direction[0][None] + spectra[2, orders:][:, :, None] * direction[1][None] + spectra[3, orders:][:, :, None] * direction[2][None]
    amp_re = load_re * inverse[None] - wavenum * (spectra[0, orders:][:, :, None] + load_im)
    amp_im = load_im * inverse[None] + wavenum * (spectra[0, :orders][:, :, None] + load_re)
    phase = wavenum * distance[None]
    cosines = jnp.cos(phase)
    sines = jnp.sin(phase)
    spreading = (inverse / (4.0 * math.pi))[None]
    real_part = lax.optimization_barrier(jnp.sum((amp_re * cosines + amp_im * sines) * spreading, axis=1))
    imag_part = lax.optimization_barrier(jnp.sum((amp_im * cosines - amp_re * sines) * spreading, axis=1))
    return jnp.concatenate([real_part, imag_part], axis=0)

def reference(flow_blocks, interp_weights, donor_owner, donor_block, panel_normals, panel_points, observer_points):
    transform = fourier_table(NT, HARM)
    global_block = (donor_owner[:, 0] * GB_DEV + donor_block).astype(jnp.int32).reshape(TILES, SLOTS)
    normals_tiled = panel_normals.reshape(3, TILES, TILE).transpose(1, 0, 2)
    points_tiled = panel_points.reshape(3, TILES, TILE).transpose(1, 0, 2)

    def one_tile(running, tile_data):
        block_ids, weight_tile, normal_tile, point_tile = tile_data
        donors = flow_blocks[block_ids].reshape(SLOTS * CB, NV * NT)
        values = jnp.dot(weight_tile, donors, preferred_element_type=jnp.float32)
        spectra = spectra_of(values, normal_tile, transform, NT)
        return (running + radiate(spectra, point_tile, observer_points), None)
    initial = jnp.zeros((2 * HARM, OBS), jnp.float32)
    running, _ = lax.scan(one_tile, initial, (global_block, interp_weights, normals_tiled, points_tiled))
    return running
```

```python
import functools
import math

import jax
import jax.numpy as jnp
import numpy as np
from jax import lax
from jax.experimental import pallas as pl
from jax.experimental.pallas import tpu as pltpu
from jax.sharding import PartitionSpec as P

NV = 5
NT = 256
HARM = 64
SERIES = 4
GROUP = 8
SLOT = 8
KAPPA = 0.5
MESH = pl.DeviceIdType.MESH


def fourier_rows(samples, orders):
    wrapped = np.arange(1, orders + 1)[:, None] * np.arange(samples)[None, :] % samples
    angles = wrapped * (2.0 * np.pi / samples)
    factor = 2.0 / samples
    return np.concatenate([factor * np.cos(angles), -factor * np.sin(angles)], axis=0).astype(np.float32)


def flip(index, bits, width):
    out = index
    bit = 1
    while bit < width:
        mine = lax.rem(index // bit, 2) if not isinstance(index, int) else (index // bit) % 2
        theirs = lax.rem(bits // bit, 2) if not isinstance(bits, int) else (bits // bit) % 2
        if not isinstance(bits, int) or theirs:
            out = out + bit * theirs * (1 - 2 * mine)
        bit *= 2
    return out


def hot(condition):
    return jnp.where(condition, 1.0, 0.0).astype(jnp.bfloat16)


def across(left, right):
    return lax.dot_general(left, right, (((1,), (1,)), ((), ())), preferred_element_type=jnp.float32)


def series_kernel(
    share,
    flow_ref,
    weight_ref,
    owner_ref,
    block_ref,
    normal_ref,
    observer_ref,
    series_ref,
    observers_ref,
    slices,
    flows,
    weights,
    facts,
    onehot,
    outgoing,
    flow_send,
    flow_recv,
    weight_send,
    weight_recv,
    fact_send,
    fact_recv,
    view_send,
    view_recv,
    series_send,
    series_recv,
):
    owners = flows.shape[0]
    held = flow_ref.shape[1]
    cells = flow_ref.shape[0]
    spread = observers_ref.shape[0]
    members = share * spread
    samples = NT // members
    width = NV * samples
    slots = weight_ref.shape[1] // cells
    me_panel = lax.axis_index("panel")
    me_obs = lax.axis_index("obs")
    sub = lax.rem(me_panel, share)
    base = me_panel - sub
    mine = me_obs * share + sub

    def member(distance):
        return {
            "panel": base + flip(sub, distance // spread, share),
            "obs": flip(me_obs, distance % spread if isinstance(distance, int) else lax.rem(distance, spread), spread),
        }

    barrier = pltpu.get_barrier_semaphore()
    for distance in range(1, members):
        pl.semaphore_signal(barrier, inc=1, device_id=member(distance), device_id_type=MESH)

    def greet(shift, carry):
        target = lax.rem(me_panel + shift, owners)
        pl.semaphore_signal(barrier, inc=1, device_id={"panel": target}, device_id_type=MESH)
        return carry

    lax.fori_loop(1, owners, greet, 0)

    quarter = share * samples
    rows = lax.broadcasted_iota(jnp.int32, (quarter, NT), 0)
    columns = lax.broadcasted_iota(jnp.int32, (quarter, NT), 1)
    pick = hot(columns == rows + me_obs * quarter)
    for cell in range(cells):
        for var in range(NV):
            piece = across(pick, flow_ref[cell, :, var * NT : (var + 1) * NT]).astype(jnp.bfloat16)
            for part in range(share):
                row = cell * width + var * samples
                slices[part, row : row + samples, :] = piece[part * samples : (part + 1) * samples, :]
    facts[0] = jnp.zeros(facts.shape[1:], jnp.float32)
    facts[0, 0:1, :] = owner_ref[...].astype(jnp.float32)
    facts[0, 1:2, :] = block_ref[...].astype(jnp.float32)
    facts[0, 2:5, :] = normal_ref[...]
    place = lax.broadcasted_iota(jnp.int32, (slots * cells, slots * cells), 0)
    goal = lax.broadcasted_iota(jnp.int32, (slots * cells, slots * cells), 1)
    turn = hot(lax.rem(place, cells) * slots + place // cells == goal)
    weights[0] = jnp.dot(weight_ref[...], turn, preferred_element_type=jnp.float32).astype(jnp.bfloat16)
    observers_ref[me_obs] = observer_ref[...]

    pl.semaphore_wait(barrier, members - 1 + owners - 1)

    def flow_copy(shift):
        target = lax.rem(me_panel + shift, owners)
        return pltpu.make_async_remote_copy(
            src_ref=slices.at[lax.rem(target, share)],
            dst_ref=flows.at[me_panel],
            send_sem=flow_send.at[shift],
            recv_sem=flow_recv.at[shift],
            device_id={"panel": target},
            device_id_type=MESH,
        )

    def push(shift, carry):
        flow_copy(shift).start()
        return carry

    lax.fori_loop(1, owners, push, 0)

    def relay(buffer, send_sem, recv_sem, held_slot, bit):
        return pltpu.make_async_remote_copy(
            src_ref=buffer.at[held_slot],
            dst_ref=buffer.at[held_slot + bit],
            send_sem=send_sem.at[held_slot + bit],
            recv_sem=recv_sem.at[held_slot + bit],
            device_id=member(bit),
            device_id_type=MESH,
        )

    bits = []
    bit = members // 2
    while bit >= 1:
        bits.append(bit)
        bit //= 2
    copies = {}

    def forward(slot):
        lowest = members if slot == 0 else slot & -slot
        for bit in bits:
            if bit < lowest:
                for kind, (buffer, send_sem, recv_sem) in enumerate(
                    ((facts, fact_send, fact_recv), (weights, weight_send, weight_recv))
                ):
                    copy = relay(buffer, send_sem, recv_sem, slot, bit)
                    copy.start()
                    copies[kind, slot + bit] = copy

    forward(0)

    def view_copy(shift):
        return pltpu.make_async_remote_copy(
            src_ref=observer_ref,
            dst_ref=observers_ref.at[me_obs],
            send_sem=view_send.at[shift],
            recv_sem=view_recv.at[shift],
            device_id={"obs": lax.rem(me_obs + shift, spread)},
            device_id_type=MESH,
        )

    views = [view_copy(shift) for shift in range(1, spread)]
    for view in views:
        view.start()
    flows[me_panel] = slices[sub]
    order = sorted(range(1, members), key=lambda slot: (bin(slot).count("1"), -slot))
    for slot in order:
        copies[0, slot].wait_recv()
        copies[1, slot].wait_recv()
        forward(slot)

    names = lax.broadcasted_iota(jnp.int32, (held, slots), 0).astype(jnp.float32)

    def mark(slot, side):
        owner_row = facts[slot, 0:1, :]
        block_row = facts[slot, 1:2, :]

        def mark_owner(owner, inner):
            row = jnp.where(owner_row == owner.astype(jnp.float32), block_row, -1.0)
            onehot[side, pl.ds(pl.multiple_of(owner * held, held), held), :] = hot(names == row)
            return inner

        lax.fori_loop(0, owners, mark_owner, 0)

    def drain(shift, carry):
        flow_copy(shift).wait()
        return carry

    lax.fori_loop(1, owners, drain, 0)

    chunk = min(owners, 8)

    def gathered(low, high):
        mark(low, 0)
        mark(high, 1)

        def partial_of(start):
            left = jnp.concatenate([flows[start + i] for i in range(chunk)], axis=1)
            row = pl.ds(pl.multiple_of(start * held, held), chunk * held)
            right = jnp.concatenate([onehot[0, row, :], onehot[1, row, :]], axis=1)
            return jnp.dot(left, right, preferred_element_type=jnp.float32)

        total = partial_of(0)
        if owners > chunk:
            total = lax.fori_loop(1, owners // chunk, lambda i, run: run + partial_of(i * chunk), total)
        return total.astype(jnp.bfloat16)

    def series_of(slot, donors):
        left = jnp.concatenate([donors[cell * width : (cell + 1) * width, :] for cell in range(cells)], axis=1)
        values = across(left, weights[slot])
        field = [values[var * samples : (var + 1) * samples, :] for var in range(NV)]
        normal = [facts[slot, 2 + i : 3 + i, :] for i in range(3)]
        flow = field[1] * normal[0] + field[2] * normal[1] + field[3] * normal[2]
        mass = (1.0 + field[0]) * flow
        return [mass] + [field[4] * normal[i] + mass * field[1 + i] for i in range(3)]

    span = pl.ds(pl.multiple_of(mine * samples, samples), samples)

    def series_copy(slot):
        return pltpu.make_async_remote_copy(
            src_ref=outgoing.at[slot],
            dst_ref=series_ref.at[:, span, :],
            send_sem=series_send.at[slot],
            recv_sem=series_recv.at[slot],
            device_id=member(slot),
            device_id_type=MESH,
        )

    def finish(slot, donors):
        for kind, term in enumerate(series_of(slot, donors)):
            outgoing[slot, kind] = term
        series_copy(slot).start()

    first = gathered(0, 1)
    for kind, term in enumerate(series_of(0, first[:, :slots])):
        series_ref[kind, span, :] = term
    finish(1, first[:, slots:])

    def pair(step, carry):
        both = gathered(2 * step, 2 * step + 1)
        finish(2 * step, both[:, :slots])
        finish(2 * step + 1, both[:, slots:])
        return carry

    lax.fori_loop(1, members // 2, pair, 0)

    for slot in range(1, members):
        copies[0, slot].wait_send()
        copies[1, slot].wait_send()
    for view in views:
        view.wait()

    def settle(slot, carry):
        series_copy(slot).wait()
        return carry

    lax.fori_loop(1, members, settle, 0)


def series_all(flow, weight, owner, block, normals, observers):
    owners = lax.axis_size("panel")
    spread = lax.axis_size("obs")
    share = max(1, min(owners, 16 // spread))
    members = share * spread
    cells, held, history = flow.shape
    panels = normals.shape[1]
    samples = NT // members
    width = NV * samples
    bf16, f32 = jnp.bfloat16, jnp.float32
    vmem = pl.BlockSpec(memory_space=pltpu.VMEM)
    dma = pltpu.SemaphoreType.DMA
    return pl.pallas_call(
        functools.partial(series_kernel, share),
        out_shape=(
            jax.ShapeDtypeStruct((SERIES, NT, panels), f32),
            jax.ShapeDtypeStruct((spread,) + observers.shape, f32),
        ),
        in_specs=[vmem] * 6,
        out_specs=(vmem, vmem),
        scratch_shapes=[
            pltpu.VMEM((share, cells * width, held), bf16),
            pltpu.VMEM((owners, cells * width, held), bf16),
            pltpu.VMEM((members,) + weight.shape, bf16),
            pltpu.VMEM((members, 8, panels), f32),
            pltpu.VMEM((2, owners * held, weight.shape[1] // cells), bf16),
            pltpu.VMEM((members, SERIES, samples, panels), f32),
            dma((owners,)),
            dma((owners,)),
            dma((members,)),
            dma((members,)),
            dma((members,)),
            dma((members,)),
            dma((spread,)),
            dma((spread,)),
            dma((members,)),
            dma((members,)),
        ],
        compiler_params=pltpu.CompilerParams(collective_id=1, has_side_effects=True, vmem_limit_bytes=60 * 1024 * 1024),
        name="series",
    )(flow, weight, owner, block, normals, observers)


def sin_cos(angle):
    turns = jnp.floor(angle * (2.0 / math.pi) + 0.5)
    reduced = angle - turns * 1.5703125
    reduced = reduced - turns * 4.837512969970703125e-4
    reduced = reduced - turns * 7.54978995489188216e-8
    square = reduced * reduced
    sine = ((-1.9515295891e-4 * square + 8.3321608736e-3) * square - 1.6666654611e-1) * square * reduced + reduced
    cosine = ((2.443315711809948e-5 * square - 1.388731625493765e-3) * square + 4.166664568298827e-2) * square * square - 0.5 * square + 1.0
    quadrant = turns.astype(jnp.int32)
    swap = (quadrant & 1) == 1
    out_sin = jnp.where(swap, cosine, sine)
    out_cos = jnp.where(swap, sine, cosine)
    out_sin = jnp.where((quadrant & 2) == 2, -out_sin, out_sin)
    out_cos = jnp.where(((quadrant + 1) & 2) == 2, -out_cos, out_cos)
    return out_sin, out_cos


def split_hi_lo(array):
    high = array.astype(jnp.bfloat16).astype(jnp.float32)
    return high, array - high


def geometry(points, observers, cos_ref, sin_ref):
    offsets = [observers[i : i + 1, :] - points[:, i : i + 1] for i in range(3)]
    squared = offsets[0] * offsets[0] + offsets[1] * offsets[1] + offsets[2] * offsets[2]
    distance = jnp.sqrt(squared)
    inverse = 1.0 / distance
    weight = inverse * (1.0 / (4.0 * math.pi))
    far = [offset * (inverse * weight) for offset in offsets]
    near = [term * inverse for term in far]
    slots = near + far + [weight, jnp.zeros_like(weight)]
    high, low = split_hi_lo(jnp.concatenate(slots, axis=0))
    right = jnp.concatenate([high, high, low, low], axis=0).astype(jnp.bfloat16)
    sine, cosine = sin_cos(KAPPA * distance)
    twice = 2.0 * cosine
    past_cos, past_sin = jnp.ones_like(cosine), jnp.zeros_like(sine)
    for order in range(8):
        cos_ref[order] = cosine
        sin_ref[order] = sine
        cosine, past_cos = twice * cosine - past_cos, cosine
        sine, past_sin = twice * sine - past_sin, sine
    return right


def amplitude(left, right, out_ref):
    lanes = lax.broadcasted_iota(jnp.int32, (1, left.shape[1]), 1) % GROUP
    masked = [left * (lanes == y).astype(jnp.float32).astype(jnp.bfloat16) for y in range(GROUP)]
    stacked = jnp.concatenate(masked, axis=0)
    out_ref[...] = jnp.dot(stacked, right, preferred_element_type=jnp.float32)


def accumulate(amp_ref, cos_ref, sin_ref, acc_ref):
    rows, observers = acc_ref.shape
    orders = rows // 2
    blocks = orders // 8
    for half in range(observers // 128):
        lane = pl.ds(half * 128, 128)
        acc_re = [acc_ref[pl.ds(8 * b, 8), lane] for b in range(blocks)]
        acc_im = [acc_ref[pl.ds(orders + 8 * b, 8), lane] for b in range(blocks)]
        for y in range(GROUP):
            cosine = cos_ref[:, y, lane]
            sine = sin_ref[:, y, lane]
            step_cos = cos_ref[7, pl.ds(y, 1), lane]
            step_sin = sin_ref[7, pl.ds(y, 1), lane]
            twice = 2.0 * step_cos
            past_cos = past_sin = None
            for b in range(blocks):
                amp_re = amp_ref[pl.ds(y * rows + 8 * b, 8), lane]
                amp_im = amp_ref[pl.ds(y * rows + orders + 8 * b, 8), lane]
                acc_re[b] = acc_re[b] + (amp_re * cosine + amp_im * sine)
                acc_im[b] = acc_im[b] + (amp_im * cosine - amp_re * sine)
                if b == 0:
                    next_cos = cosine * step_cos - sine * step_sin
                    next_sin = sine * step_cos + cosine * step_sin
                else:
                    next_cos = twice * cosine - past_cos
                    next_sin = twice * sine - past_sin
                past_cos, past_sin, cosine, sine = cosine, sine, next_cos, next_sin
        for b in range(blocks):
            acc_ref[pl.ds(8 * b, 8), lane] = acc_re[b]
            acc_ref[pl.ds(orders + 8 * b, 8), lane] = acc_im[b]


def radiate_kernel(
    series_ref,
    table_ref,
    point_ref,
    observers_ref,
    out_ref,
    terms,
    points,
    lefts,
    acc_ref,
    amp_a,
    amp_b,
    cos_a,
    cos_b,
    sin_a,
    sin_b,
    outgoing,
    arrived,
    send_sem,
    recv_sem,
):
    owners = lax.axis_size("panel")
    spread = lax.axis_size("obs")
    me_panel = lax.axis_index("panel")
    me_obs = lax.axis_index("obs")
    orders = acc_ref.shape[0] // 2
    panels = point_ref.shape[1]
    groups = panels // GROUP
    rows = out_ref.shape[0]
    barrier = pltpu.get_barrier_semaphore()
    for turn in range(spread):

        def greet(shift, carry):
            pl.semaphore_signal(
                barrier,
                inc=1,
                device_id={"panel": lax.rem(me_panel + shift, owners), "obs": lax.rem(me_obs + turn, spread)},
                device_id_type=MESH,
            )
            return carry

        lax.fori_loop(1 if turn == 0 else 0, owners, greet, 0)

    points[...] = jnp.zeros_like(points)
    points[0:3, :] = point_ref[...]
    points[...] = jnp.transpose(points[...])
    wavenum = KAPPA * (1 + lax.broadcasted_iota(jnp.int32, (orders, panels), 0)).astype(jnp.float32)
    for kind in range(SERIES):
        near = jnp.dot(
            table_ref[...], series_ref[kind], preferred_element_type=jnp.float32, precision=lax.Precision.HIGHEST
        )
        far = jnp.concatenate([-wavenum * near[orders:], wavenum * near[:orders]], axis=0)
        if kind == 0:
            terms[6] = far
        else:
            terms[kind - 1] = near
            terms[kind + 2] = far
    lane = lax.broadcasted_iota(jnp.int32, (2 * orders, panels), 1)

    @pl.loop(0, groups)
    def _(group):
        both = jnp.zeros((2 * orders, panels), jnp.float32)
        for slot in range(SLOT - 1):
            moved = pltpu.roll(terms[slot], lax.rem(panels + (slot - group) * GROUP, panels), 1)
            both = jnp.where(lane // GROUP == slot, moved, both)
        high, low = split_hi_lo(both)
        lefts[group] = jnp.where(lane < SLOT * GROUP, high, pltpu.roll(low, SLOT * GROUP, 1)).astype(jnp.bfloat16)

    pl.semaphore_wait(barrier, owners * spread - 1)

    def left_of(group):
        left = lefts[group]
        return jnp.concatenate([left, left], axis=1)

    def points_at(group):
        return points[pl.ds(pl.multiple_of(group * GROUP, GROUP), GROUP), :]

    def term_copy(step, shift):
        slot = lax.rem(step + 1, spread) * owners + shift
        target = lax.rem(me_panel + shift, owners)
        return pltpu.make_async_remote_copy(
            src_ref=outgoing.at[step, target],
            dst_ref=arrived.at[slot],
            send_sem=send_sem.at[slot],
            recv_sem=recv_sem.at[slot],
            device_id={"panel": target, "obs": lax.rem(me_obs + step + 1, spread)},
            device_id_type=MESH,
        )

    @pl.loop(0, spread)
    def _(step):
        observers = observers_ref[lax.rem(me_obs + step + 1, spread)]
        acc_ref[...] = jnp.zeros_like(acc_ref)
        amplitude(left_of(0), geometry(points_at(0), observers, cos_a, sin_a), amp_a)

        @pl.loop(0, groups // 2)
        def _(pair):
            amplitude(left_of(2 * pair + 1), geometry(points_at(2 * pair + 1), observers, cos_b, sin_b), amp_b)
            accumulate(amp_a, cos_a, sin_a, acc_ref)
            after = jnp.minimum(pair + 1, groups // 2 - 1)
            amplitude(left_of(2 * after), geometry(points_at(2 * after), observers, cos_a, sin_a), amp_a)
            accumulate(amp_b, cos_b, sin_b, acc_ref)

        for owner in range(owners):
            outgoing[step, owner] = acc_ref[owner * rows : (owner + 1) * rows, :]

        @pl.when(step < spread - 1)
        def _():
            term_copy(step, 0).start()

        def push(shift, carry):
            term_copy(step, shift).start()
            return carry

        lax.fori_loop(1, owners, push, 0)

    arrived[0] = outgoing[spread - 1, me_panel]
    for step in range(spread):

        def settle(shift, carry):
            term_copy(step, shift).wait()
            return carry

        lax.fori_loop(1 if step == spread - 1 else 0, owners, settle, 0)

    def add(slot, total):
        return total + arrived[slot]

    out_ref[...] = lax.fori_loop(1, owners * spread, add, arrived[0])


def radiate_all(series, points, observers):
    owners = lax.axis_size("panel")
    spread = lax.axis_size("obs")
    panels = points.shape[1]
    count = observers.shape[2]
    rows = 2 * HARM // owners
    f32 = jnp.float32
    wave = pltpu.VMEM((8, GROUP, count), f32)
    amp = pltpu.VMEM((GROUP * 2 * HARM, count), f32)
    return pl.pallas_call(
        radiate_kernel,
        out_shape=jax.ShapeDtypeStruct((rows, count), f32),
        in_specs=[pl.BlockSpec(memory_space=pltpu.VMEM)] * 4,
        out_specs=pl.BlockSpec(memory_space=pltpu.VMEM),
        scratch_shapes=[
            pltpu.VMEM((SLOT - 1, 2 * HARM, panels), f32),
            pltpu.VMEM((panels, panels), f32),
            pltpu.VMEM((panels // GROUP, 2 * HARM, panels), jnp.bfloat16),
            pltpu.VMEM((2 * HARM, count), f32),
            amp,
            amp,
            wave,
            wave,
            wave,
            wave,
            pltpu.VMEM((spread, owners, rows, count), f32),
            pltpu.VMEM((spread * owners, rows, count), f32),
            pltpu.SemaphoreType.DMA((spread * owners,)),
            pltpu.SemaphoreType.DMA((spread * owners,)),
        ],
        compiler_params=pltpu.CompilerParams(collective_id=2, has_side_effects=True, vmem_limit_bytes=60 * 1024 * 1024),
        name="radiate",
    )(series, jnp.asarray(fourier_rows(NT, HARM)), points, observers)


def body(
    flow_blocks,
    interp_weights,
    donor_owner,
    donor_block,
    panel_normals,
    panel_points,
    observer_points,
):
    tiles, width, stencil = interp_weights.shape
    series, observers = series_all(
        flow_blocks.transpose(1, 0, 2),
        interp_weights.reshape(tiles * width, stencil),
        donor_owner.reshape(1, -1),
        donor_block.reshape(1, -1),
        panel_normals,
        observer_points,
    )
    return radiate_all(series, panel_points, observers)


def solution(mesh):
    return jax.shard_map(
        body,
        mesh=mesh,
        in_specs=(
            P("panel", None, None),
            P(("panel", "obs"), None, None),
            P(("panel", "obs"), None),
            P(("panel", "obs")),
            P(None, ("panel", "obs")),
            P(None, ("panel", "obs")),
            P(None, "obs"),
        ),
        out_specs=P("panel", "obs"),
        check_vma=False,
    )
```

```python
import functools
import math

import jax
import jax.numpy as jnp
import numpy as np
from jax import lax
from jax.experimental import pallas as pl
from jax.experimental.pallas import tpu as pltpu
from jax.sharding import PartitionSpec as P

NV = 5
NT = 256
HARM = 64
SERIES = 4
GROUP = 8
SLOT = 8
KAPPA = 0.5
MESH = pl.DeviceIdType.MESH


def fourier_rows(samples, orders):
    wrapped = np.arange(1, orders + 1)[:, None] * np.arange(samples)[None, :] % samples
    angles = wrapped * (2.0 * np.pi / samples)
    factor = 2.0 / samples
    return np.concatenate([factor * np.cos(angles), -factor * np.sin(angles)], axis=0).astype(np.float32)


def three_parts(table):
    parts = []
    rest = table.astype(np.float64)
    for _ in range(3):
        part = rest.astype(jnp.bfloat16)
        parts.append(part)
        rest = rest - part.astype(np.float64)
    return np.stack(parts)


def flip(index, bits, width):
    out = index
    bit = 1
    while bit < width:
        mine = lax.rem(index // bit, 2) if not isinstance(index, int) else (index // bit) % 2
        theirs = lax.rem(bits // bit, 2) if not isinstance(bits, int) else (bits // bit) % 2
        if not isinstance(bits, int) or theirs:
            out = out + bit * theirs * (1 - 2 * mine)
        bit *= 2
    return out


def hot(condition):
    return jnp.where(condition, 1.0, 0.0).astype(jnp.bfloat16)


def product(acc, unit, lefts, rights, transpose=False):
    for turn, (left, right) in enumerate(zip(lefts, rights)):
        pltpu.matmul_push_rhs(right, staging_register=turn % 2, mxu_index=unit, transpose=transpose)
        pltpu.matmul_acc_lhs(acc, left, load_staged_rhs=turn % 2)
    return pltpu.matmul_pop(acc)


def sin_cos(angle):
    turns = jnp.floor(angle * (2.0 / math.pi) + 0.5)
    reduced = angle - turns * 1.5703125
    reduced = reduced - turns * 4.837512969970703125e-4
    reduced = reduced - turns * 7.54978995489188216e-8
    square = reduced * reduced
    sine = ((-1.9515295891e-4 * square + 8.3321608736e-3) * square - 1.6666654611e-1) * square * reduced + reduced
    cosine = ((2.443315711809948e-5 * square - 1.388731625493765e-3) * square + 4.166664568298827e-2) * square * square - 0.5 * square + 1.0
    quadrant = turns.astype(jnp.int32)
    swap = (quadrant & 1) == 1
    out_sin = jnp.where(swap, cosine, sine)
    out_cos = jnp.where(swap, sine, cosine)
    out_sin = jnp.where((quadrant & 2) == 2, -out_sin, out_sin)
    out_cos = jnp.where(((quadrant + 1) & 2) == 2, -out_cos, out_cos)
    return out_sin, out_cos


def split_hi_lo(array):
    high = array.astype(jnp.bfloat16).astype(jnp.float32)
    return high, array - high


def geometry(points, observers, right_ref, cos_ref, sin_ref):
    offsets = [observers[i : i + 1, :] - points[:, i : i + 1] for i in range(3)]
    squared = offsets[0] * offsets[0] + offsets[1] * offsets[1] + offsets[2] * offsets[2]
    distance = jnp.sqrt(squared)
    inverse = 1.0 / distance
    weight = inverse * (1.0 / (4.0 * math.pi))
    far = [offset * (inverse * weight) for offset in offsets]
    near = [term * inverse for term in far]
    slots = near + far + [weight, jnp.zeros_like(weight)]
    high, low = split_hi_lo(jnp.concatenate(slots, axis=0))
    right_ref[...] = jnp.concatenate([high, low], axis=0).astype(jnp.bfloat16)
    sine, cosine = sin_cos(KAPPA * distance)
    twice = 2.0 * cosine
    past_cos, past_sin = jnp.ones_like(cosine), jnp.zeros_like(sine)
    for order in range(8):
        cos_ref[:, order, :] = cosine
        sin_ref[:, order, :] = sine
        cosine, past_cos = twice * cosine - past_cos, cosine
        sine, past_sin = twice * sine - past_sin, sine


def load_right(right_ref):
    half = right_ref.shape[0] // 2
    high, low = right_ref[:half, :], right_ref[half:, :]
    right = jnp.concatenate([high, high, low, low], axis=0)
    for unit in range(2):
        pltpu.matmul_push_rhs(right, staging_register=0, mxu_index=unit)


def amplitude(acc, y, left, fresh):
    lanes = lax.rem(lax.broadcasted_iota(jnp.int32, (1, left.shape[1]), 1), GROUP)
    one = left * (lanes == y).astype(jnp.float32).astype(jnp.bfloat16)
    both = jnp.concatenate([one, one], axis=1)
    pltpu.matmul_acc_lhs(acc, both, load_staged_rhs=0 if fresh else None)


def accumulate(amp, cosine, sine, step_cos, step_sin, acc_re, acc_im):
    blocks = len(acc_re)
    orders = amp.shape[0] // 2
    twice = 2.0 * step_cos
    past_cos = past_sin = None
    for b in range(blocks):
        amp_re = amp[8 * b : 8 * b + 8, :]
        amp_im = amp[orders + 8 * b : orders + 8 * b + 8, :]
        acc_re[b] = acc_re[b] + (amp_re * cosine + amp_im * sine)
        acc_im[b] = acc_im[b] + (amp_im * cosine - amp_re * sine)
        if b == 0:
            next_cos = cosine * step_cos - sine * step_sin
            next_sin = sine * step_cos + cosine * step_sin
        else:
            next_cos = twice * cosine - past_cos
            next_sin = twice * sine - past_sin
        past_cos, past_sin, cosine, sine = cosine, sine, next_cos, next_sin


def whole_kernel(
    share,
    flow_ref,
    weight_ref,
    owner_ref,
    block_ref,
    normal_ref,
    point_ref,
    observer_ref,
    table_ref,
    out_ref,
    slices,
    flows,
    weights,
    facts,
    onehot,
    outgoing,
    series_ref,
    observers_ref,
    points,
    rights,
    cosines,
    sines,
    terms,
    lefts,
    acc_ref,
    sums,
    arrived,
    flow_send,
    flow_recv,
    weight_send,
    weight_recv,
    fact_send,
    fact_recv,
    view_send,
    view_recv,
    series_send,
    series_recv,
    term_send,
    term_recv,
):
    owners = flows.shape[0]
    held = flow_ref.shape[1]
    cells = flow_ref.shape[0]
    spread = observers_ref.shape[0]
    members = share * spread
    samples = NT // members
    width = NV * samples
    slots = weight_ref.shape[1] // cells
    me_panel = lax.axis_index("panel")
    me_obs = lax.axis_index("obs")
    sub = lax.rem(me_panel, share)
    base = me_panel - sub
    mine = me_obs * share + sub

    def member(distance):
        return {
            "panel": base + flip(sub, distance // spread, share),
            "obs": flip(me_obs, distance % spread if isinstance(distance, int) else lax.rem(distance, spread), spread),
        }

    orders = acc_ref.shape[0] // 2
    panels = point_ref.shape[1]
    groups = panels // GROUP
    rows_out = out_ref.shape[0]
    ahead = onehot.shape[0] == members
    barrier = pltpu.get_barrier_semaphore()
    for turn in range(spread):

        def greet(shift, carry):
            pl.semaphore_signal(
                barrier,
                inc=1,
                device_id={"panel": lax.rem(me_panel + shift, owners), "obs": lax.rem(me_obs + turn, spread)},
                device_id_type=MESH,
            )
            return carry

        lax.fori_loop(1 if turn == 0 else 0, owners, greet, 0)

    def prepare(*accs):
        quarters, squares, talls, middles = accs[0:4], accs[4:6], accs[6:8], accs[8:10]
        quarter = share * samples
        rows = lax.broadcasted_iota(jnp.int32, (quarter, NT), 0)
        columns = lax.broadcasted_iota(jnp.int32, (quarter, NT), 1)
        pick = hot(columns == rows + me_obs * quarter)
        for turn, (cell, var) in enumerate((cell, var) for cell in range(0, cells, 2) for var in range(NV)):
            span = slice(var * NT, (var + 1) * NT)
            right = jnp.concatenate([flow_ref[cell, :, span], flow_ref[cell + 1, :, span]], axis=0)
            piece = product(quarters[turn % 4], turn % 2, [pick], [right], True).astype(jnp.bfloat16)
            for side in range(2):
                for part in range(share):
                    row = (cell + side) * width + var * samples
                    slices[part, row : row + samples, :] = piece[
                        part * samples : (part + 1) * samples, side * held : (side + 1) * held
                    ]
        facts[0] = jnp.zeros(facts.shape[1:], jnp.float32)
        facts[0, 0:1, :] = owner_ref[...].astype(jnp.float32)
        facts[0, 1:2, :] = block_ref[...].astype(jnp.float32)
        facts[0, 2:5, :] = normal_ref[...]
        place = lax.broadcasted_iota(jnp.int32, (slots * cells, slots * cells), 0)
        goal = lax.broadcasted_iota(jnp.int32, (slots * cells, slots * cells), 1)
        turn = hot(lax.rem(place, cells) * slots + place // cells == goal)
        for unit in range(2):
            span = slice(unit * 256, (unit + 1) * 256)
            tiles = [weight_ref[:, :256], weight_ref[:, 256:]]
            weights[0, :, span] = product(squares[unit], unit, tiles, [turn[:256, span], turn[256:, span]]).astype(jnp.bfloat16)
        observers_ref[me_obs] = observer_ref[...]

        points[...] = jnp.zeros_like(points)
        points[0:3, :] = point_ref[...]
        points[...] = jnp.transpose(points[...])

        pl.semaphore_wait(barrier, owners * spread - 1)

        def flow_copy(shift):
            target = flip(me_panel, shift, owners)
            return pltpu.make_async_remote_copy(
                src_ref=slices.at[lax.rem(target, share)],
                dst_ref=flows.at[me_panel],
                send_sem=flow_send.at[shift],
                recv_sem=flow_recv.at[shift],
                device_id={"panel": target},
                device_id_type=MESH,
            )

        def push(turn, carry):
            flow_copy(owners - turn).start()
            return carry

        def relay(buffer, send_sem, recv_sem, held_slot, bit):
            return pltpu.make_async_remote_copy(
                src_ref=buffer.at[held_slot],
                dst_ref=buffer.at[held_slot + bit],
                send_sem=send_sem.at[held_slot + bit],
                recv_sem=recv_sem.at[held_slot + bit],
                device_id=member(bit),
                device_id_type=MESH,
            )

        copies = {}

        def forward(slot):
            inner = slot % spread
            lowest = inner & -inner if inner else spread
            steps = [part * spread for part in range(1, share)] if slot == 0 else []
            bit = spread // 2
            while bit >= 1:
                steps.append(bit)
                bit //= 2
            for bit in steps:
                if bit < lowest or bit >= spread:
                    for kind, (buffer, send_sem, recv_sem) in enumerate(
                        ((facts, fact_send, fact_recv), (weights, weight_send, weight_recv))
                    ):
                        copy = relay(buffer, send_sem, recv_sem, slot, bit)
                        copy.start()
                        copies[kind, slot + bit] = copy

        forward(0)
        lax.fori_loop(1, owners, push, 0)

        def view_copy(shift):
            return pltpu.make_async_remote_copy(
                src_ref=observer_ref,
                dst_ref=observers_ref.at[me_obs],
                send_sem=view_send.at[shift],
                recv_sem=view_recv.at[shift],
                device_id={"obs": lax.rem(me_obs + shift, spread)},
                device_id_type=MESH,
            )

        views = [view_copy(shift) for shift in range(1, spread)]
        for view in views:
            view.start()
        flows[me_panel] = slices[sub]

        def survey(step):
            observers = observers_ref[lax.rem(me_obs + step + 1, spread)]

            @pl.loop(0, groups)
            def _(group):
                place = step * groups + group
                near = points[pl.ds(pl.multiple_of(group * GROUP, GROUP), GROUP), :]
                geometry(near, observers, rights.at[place], cosines.at[place], sines.at[place])

        def receive(slots_now):
            for slot in slots_now:
                copies[0, slot].wait_recv()
                copies[1, slot].wait_recv()
                forward(slot)

        order = sorted(
            range(1, members),
            key=lambda slot: (bin(slot % spread).count("1"), -(slot % spread), bin(slot).count("1"), -slot),
        )
        direct = share - 1
        survey(spread - 1)
        receive(order[:direct])
        for view in views:
            view.wait()
        for step in range(spread - 1):
            if step == 1:
                receive(order[direct : direct + share])
            survey(step)
        receive(order[direct + share :])

        names = lax.broadcasted_iota(jnp.int32, (held, slots), 0).astype(jnp.float32)

        def mark(slot, side):
            owner_row = facts[slot, 0:1, :]
            block_row = facts[slot, 1:2, :]

            def mark_owner(owner, inner):
                row = jnp.where(owner_row == owner.astype(jnp.float32), block_row, -1.0)
                onehot[side, pl.ds(pl.multiple_of(owner * held, held), held), :] = hot(names == row)
                return inner

            lax.fori_loop(0, owners, mark_owner, 0)

        if ahead:

            @pl.loop(0, members)
            def _(slot):
                mark(slot, slot)

        def drain(shift, carry):
            flow_copy(shift).wait()
            return carry

        lax.fori_loop(1, owners, drain, 0)

        chunk = min(owners, 8)

        def gathered(low, high):
            if not ahead:
                mark(low, 0)
                mark(high, 1)
            sides = (low, high) if ahead else (0, 1)

            def partial_of(start):
                terms_of = []
                for unit in range(2):
                    some = range(unit * chunk // 2, (unit + 1) * chunk // 2, 2)
                    left = [jnp.concatenate([flows[start + i], flows[start + i + 1]], axis=1) for i in some]
                    right = []
                    for i in some:
                        row = pl.ds(pl.multiple_of((start + i) * held, held), 2 * held)
                        right.append(jnp.concatenate([onehot[sides[0], row, :], onehot[sides[1], row, :]], axis=1))
                    terms_of.append(product(talls[unit], unit, left, right))
                return terms_of[0] + terms_of[1]

            total = partial_of(0)
            if owners > chunk:
                total = lax.fori_loop(1, owners // chunk, lambda i, run: run + partial_of(i * chunk), total)
            return total.astype(jnp.bfloat16)

        def values_of(low, high, donors):
            terms_of = []
            for unit in range(2):
                pairs = range(unit * cells // 2, (unit + 1) * cells // 2)
                left = []
                for side in range(2):
                    lanes = slice(side * slots, (side + 1) * slots)
                    left.append(jnp.concatenate([donors[cell * width : (cell + 1) * width, lanes] for cell in pairs], axis=1))
                span = slice(unit * 256, (unit + 1) * 256)
                right = jnp.concatenate([weights[low, :, span], weights[high, :, span]], axis=0)
                terms_of.append(product(middles[unit], unit, [jnp.concatenate(left, axis=0)], [right], True))
            both = terms_of[0] + terms_of[1]
            return both[:width, :panels], both[width:, panels:]

        def series_of(slot, values):
            field = [values[var * samples : (var + 1) * samples, :] for var in range(NV)]
            normal = [facts[slot, 2 + i : 3 + i, :] for i in range(3)]
            flow = field[1] * normal[0] + field[2] * normal[1] + field[3] * normal[2]
            mass = (1.0 + field[0]) * flow
            return [mass] + [field[4] * normal[i] + mass * field[1 + i] for i in range(3)]

        span = pl.ds(pl.multiple_of(mine * samples, samples), samples)

        def series_copy(slot):
            return pltpu.make_async_remote_copy(
                src_ref=outgoing.at[slot],
                dst_ref=series_ref.at[:, span, :],
                send_sem=series_send.at[slot],
                recv_sem=series_recv.at[slot],
                device_id=member(slot),
                device_id_type=MESH,
            )

        def finish(slot, values):
            for kind, term in enumerate(series_of(slot, values)):
                outgoing[slot, kind] = term
            series_copy(slot).start()

        low_values, high_values = values_of(0, 1, gathered(0, 1))
        for kind, term in enumerate(series_of(0, low_values)):
            series_ref[kind, span, :] = term
        finish(1, high_values)

        def pair(step, carry):
            low, high = 2 * step, 2 * step + 1
            first_values, second_values = values_of(low, high, gathered(low, high))
            finish(low, first_values)
            finish(high, second_values)
            return carry

        lax.fori_loop(1, members // 2, pair, 0)

        for slot in range(1, members):
            copies[0, slot].wait_send()
            copies[1, slot].wait_send()

        def settle_series(slot, carry):
            series_copy(slot).wait()
            return carry

        lax.fori_loop(1, members, settle_series, 0)

        wavenum = KAPPA * (1 + lax.broadcasted_iota(jnp.int32, (orders, panels), 0)).astype(jnp.float32)
        for unit in range(2):
            rest = jnp.concatenate([series_ref[2 * unit], series_ref[2 * unit + 1]], axis=1)
            left, right = [], []
            for depth in range(3):
                part = rest.astype(jnp.bfloat16)
                rest = rest - part.astype(jnp.float32)
                for level in range(3 - depth):
                    left.append(table_ref[level])
                    right.append(part)
            both = product(squares[unit], unit, left, right)
            for side in range(2):
                kind = 2 * unit + side
                near = both[:, side * panels : (side + 1) * panels]
                far = jnp.concatenate([-wavenum * near[orders:], wavenum * near[:orders]], axis=0)
                if kind == 0:
                    terms[6] = far
                else:
                    terms[kind - 1] = near
                    terms[kind + 2] = far
        lane = lax.broadcasted_iota(jnp.int32, (2 * orders, panels), 1)

        @pl.loop(0, groups)
        def _(group):
            both = jnp.zeros((2 * orders, panels), jnp.float32)
            for slot in range(SLOT - 1):
                moved = pltpu.roll(terms[slot], lax.rem(panels + (slot - group) * GROUP, panels), 1)
                both = jnp.where(lane // GROUP == slot, moved, both)
            high, low = split_hi_lo(both)
            lefts[group] = jnp.where(lane < SLOT * GROUP, high, pltpu.roll(low, SLOT * GROUP, 1)).astype(jnp.bfloat16)


    def term_copy(step, shift):
        slot = lax.rem(step + 1, spread) * owners + shift
        target = lax.rem(me_panel + shift, owners)
        return pltpu.make_async_remote_copy(
            src_ref=sums.at[step, target],
            dst_ref=arrived.at[slot],
            send_sem=term_send.at[slot],
            recv_sem=term_recv.at[slot],
            device_id={"panel": target, "obs": lax.rem(me_obs + step + 1, spread)},
            device_id_type=MESH,
        )

    def radiate(*accs):

        @pl.loop(0, spread)
        def _(step):
            first = step * groups
            acc_ref[...] = jnp.zeros_like(acc_ref)
            load_right(rights.at[first])
            for y in range(GROUP):
                amplitude(accs[y], y, lefts[0], y < 2)

            @pl.loop(0, groups)
            def _(group):
                place = first + group
                after = jnp.minimum(group + 1, groups - 1)
                load_right(rights.at[first + after])
                blocks = orders // 8
                acc_re = [acc_ref[pl.ds(8 * b, 8), :] for b in range(blocks)]
                acc_im = [acc_ref[pl.ds(orders + 8 * b, 8), :] for b in range(blocks)]
                left = lefts[after]
                for y in range(GROUP):
                    amp = pltpu.matmul_pop(accs[y])
                    amplitude(accs[y], y, left, y < 2)
                    steps = (cosines[place, y, 7:8, :], sines[place, y, 7:8, :])
                    accumulate(amp, cosines[place, y], sines[place, y], *steps, acc_re, acc_im)
                for b in range(blocks):
                    acc_ref[pl.ds(8 * b, 8), :] = acc_re[b]
                    acc_ref[pl.ds(orders + 8 * b, 8), :] = acc_im[b]

            for acc in accs:
                pltpu.matmul_pop(acc)

            for owner in range(owners):
                sums[step, owner] = acc_ref[owner * rows_out : (owner + 1) * rows_out, :]

            @pl.when(step < spread - 1)
            def _():
                term_copy(step, 0).start()

            def push(shift, carry):
                term_copy(step, shift).start()
                return carry

            lax.fori_loop(1, owners, push, 0)

    def store(unit, height):
        return pltpu.ACC(unit)((height, 256), jnp.float32)

    part_rows = share * samples
    pl.run_scoped(
        prepare,
        *[store(turn % 2, part_rows) for turn in range(4)],
        *[store(unit, 2 * orders) for unit in range(2)],
        *[store(unit, cells * width) for unit in range(2)],
        *[store(unit, 2 * width) for unit in range(2)],
    )
    pl.run_scoped(radiate, *[store(y % 2, 2 * orders) for y in range(GROUP)])

    arrived[0] = sums[spread - 1, me_panel]
    for step in range(spread):

        def settle(shift, carry):
            term_copy(step, shift).wait()
            return carry

        lax.fori_loop(1 if step == spread - 1 else 0, owners, settle, 0)

    def add(slot, total):
        return total + arrived[slot]

    out_ref[...] = lax.fori_loop(1, owners * spread, add, arrived[0])


def run(flow, weight, owner, block, normals, points, observers):
    owners = lax.axis_size("panel")
    spread = lax.axis_size("obs")
    share = max(1, min(owners, 16 // spread))
    members = share * spread
    cells, held, history = flow.shape
    panels = normals.shape[1]
    count = observers.shape[1]
    samples = NT // members
    width = NV * samples
    slots = weight.shape[1] // cells
    places = spread * (panels // GROUP)
    rows = 2 * HARM // owners
    ahead = members * owners * held * slots <= 1 << 22
    bf16, f32 = jnp.bfloat16, jnp.float32
    vmem = pl.BlockSpec(memory_space=pltpu.VMEM)
    dma = pltpu.SemaphoreType.DMA
    wave = pltpu.VMEM((places, GROUP, 8, count), f32)
    return pl.pallas_call(
        functools.partial(whole_kernel, share),
        out_shape=jax.ShapeDtypeStruct((rows, count), f32),
        in_specs=[vmem] * 8,
        out_specs=vmem,
        scratch_shapes=[
            pltpu.VMEM((share, cells * width, held), bf16),
            pltpu.VMEM((owners, cells * width, held), bf16),
            pltpu.VMEM((members,) + weight.shape, bf16),
            pltpu.VMEM((members, 8, panels), f32),
            pltpu.VMEM((members if ahead else 2, owners * held, slots), bf16),
            pltpu.VMEM((members, SERIES, samples, panels), f32),
            pltpu.VMEM((SERIES, NT, panels), f32),
            pltpu.VMEM((spread,) + observers.shape, f32),
            pltpu.VMEM((panels, panels), f32),
            pltpu.VMEM((places, 2 * SLOT * GROUP, count), bf16),
            wave,
            wave,
            pltpu.VMEM((SLOT - 1, 2 * HARM, panels), f32),
            pltpu.VMEM((panels // GROUP, 2 * HARM, panels), bf16),
            pltpu.VMEM((2 * HARM, count), f32),
            pltpu.VMEM((spread, owners, rows, count), f32),
            pltpu.VMEM((spread * owners, rows, count), f32),
            dma((owners,)),
            dma((owners,)),
            dma((members,)),
            dma((members,)),
            dma((members,)),
            dma((members,)),
            dma((spread,)),
            dma((spread,)),
            dma((members,)),
            dma((members,)),
            dma((spread * owners,)),
            dma((spread * owners,)),
        ],
        compiler_params=pltpu.CompilerParams(
            collective_id=1,
            has_side_effects=True,
            vmem_limit_bytes=63000 * 1024,
        ),
        name="whole",
    )(flow, weight, owner, block, normals, points, observers, jnp.asarray(three_parts(fourier_rows(NT, HARM))))


def body(
    flow_blocks,
    interp_weights,
    donor_owner,
    donor_block,
    panel_normals,
    panel_points,
    observer_points,
):
    tiles, width, stencil = interp_weights.shape
    return run(
        flow_blocks.transpose(1, 0, 2),
        interp_weights.reshape(tiles * width, stencil),
        donor_owner.reshape(1, -1),
        donor_block.reshape(1, -1),
        panel_normals,
        panel_points,
        observer_points,
    )


def solution(mesh):
    return jax.shard_map(
        body,
        mesh=mesh,
        in_specs=(
            P("panel", None, None),
            P(("panel", "obs"), None, None),
            P(("panel", "obs"), None),
            P(("panel", "obs")),
            P(None, ("panel", "obs")),
            P(None, ("panel", "obs")),
            P(None, "obs"),
        ),
        out_specs=P("panel", "obs"),
        check_vma=False,
    )
```

```python
import functools
import math

import jax
import jax.numpy as jnp
import numpy as np
from jax import lax
from jax.experimental import pallas as pl
from jax.experimental.pallas import tpu as pltpu
from jax.sharding import PartitionSpec as P

NV = 5
NT = 256
HARM = 64
SERIES = 4
GROUP = 8
SLOT = 8
KAPPA = 0.5
MESH = pl.DeviceIdType.MESH


def fourier_rows(samples, orders):
    wrapped = np.arange(1, orders + 1)[:, None] * np.arange(samples)[None, :] % samples
    angles = wrapped * (2.0 * np.pi / samples)
    factor = 2.0 / samples
    return np.concatenate([factor * np.cos(angles), -factor * np.sin(angles)], axis=0).astype(np.float32)


def three_parts(table):
    parts = []
    rest = table.astype(np.float64)
    for _ in range(3):
        part = rest.astype(jnp.bfloat16)
        parts.append(part)
        rest = rest - part.astype(np.float64)
    return np.stack(parts)


def flip(index, bits, width):
    out = index
    bit = 1
    while bit < width:
        mine = lax.rem(index // bit, 2) if not isinstance(index, int) else (index // bit) % 2
        theirs = lax.rem(bits // bit, 2) if not isinstance(bits, int) else (bits // bit) % 2
        if not isinstance(bits, int) or theirs:
            out = out + bit * theirs * (1 - 2 * mine)
        bit *= 2
    return out


def hot(condition):
    return jnp.where(condition, 1.0, 0.0).astype(jnp.bfloat16)


def product(acc, unit, lefts, rights, transpose=False):
    for turn, (left, right) in enumerate(zip(lefts, rights)):
        pltpu.matmul_push_rhs(right, staging_register=turn % 2, mxu_index=unit, transpose=transpose)
        pltpu.matmul_acc_lhs(acc, left, load_staged_rhs=turn % 2)
    return pltpu.matmul_pop(acc)


def sin_cos(angle):
    turns = jnp.floor(angle * (2.0 / math.pi) + 0.5)
    reduced = angle - turns * 1.5703125
    reduced = reduced - turns * 4.837512969970703125e-4
    reduced = reduced - turns * 7.54978995489188216e-8
    square = reduced * reduced
    sine = ((-1.9515295891e-4 * square + 8.3321608736e-3) * square - 1.6666654611e-1) * square * reduced + reduced
    cosine = ((2.443315711809948e-5 * square - 1.388731625493765e-3) * square + 4.166664568298827e-2) * square * square - 0.5 * square + 1.0
    quadrant = turns.astype(jnp.int32)
    swap = (quadrant & 1) == 1
    out_sin = jnp.where(swap, cosine, sine)
    out_cos = jnp.where(swap, sine, cosine)
    out_sin = jnp.where((quadrant & 2) == 2, -out_sin, out_sin)
    out_cos = jnp.where(((quadrant + 1) & 2) == 2, -out_cos, out_cos)
    return out_sin, out_cos


def split_hi_lo(array):
    high = array.astype(jnp.bfloat16).astype(jnp.float32)
    return high, array - high


def geometry(points, observers, right_ref, cos_ref, sin_ref):
    offsets = [observers[i : i + 1, :] - points[:, i : i + 1] for i in range(3)]
    squared = offsets[0] * offsets[0] + offsets[1] * offsets[1] + offsets[2] * offsets[2]
    distance = jnp.sqrt(squared)
    inverse = 1.0 / distance
    weight = inverse * (1.0 / (4.0 * math.pi))
    far = [offset * (inverse * weight) for offset in offsets]
    near = [term * inverse for term in far]
    slots = near + far + [weight, jnp.zeros_like(weight)]
    high, low = split_hi_lo(jnp.concatenate(slots, axis=0))
    right_ref[...] = jnp.concatenate([high, low], axis=0).astype(jnp.bfloat16)
    sine, cosine = sin_cos(KAPPA * distance)
    twice = 2.0 * cosine
    past_cos, past_sin = jnp.ones_like(cosine), jnp.zeros_like(sine)
    for order in range(8):
        cos_ref[:, order, :] = cosine
        sin_ref[:, order, :] = sine
        cosine, past_cos = twice * cosine - past_cos, cosine
        sine, past_sin = twice * sine - past_sin, sine


def load_right(right_ref):
    half = right_ref.shape[0] // 2
    high, low = right_ref[:half, :], right_ref[half:, :]
    right = jnp.concatenate([high, high, low, low], axis=0)
    for unit in range(2):
        pltpu.matmul_push_rhs(right, staging_register=0, mxu_index=unit)


def amplitude(acc, y, left, fresh):
    lanes = lax.rem(lax.broadcasted_iota(jnp.int32, (1, left.shape[1]), 1), GROUP)
    one = left * (lanes == y).astype(jnp.float32).astype(jnp.bfloat16)
    both = jnp.concatenate([one, one], axis=1)
    pltpu.matmul_acc_lhs(acc, both, load_staged_rhs=0 if fresh else None)


def accumulate(amp, cosine, sine, step_cos, step_sin, acc_re, acc_im):
    blocks = len(acc_re)
    orders = amp.shape[0] // 2
    twice = 2.0 * step_cos
    past_cos = past_sin = None
    for b in range(blocks):
        amp_re = amp[8 * b : 8 * b + 8, :]
        amp_im = amp[orders + 8 * b : orders + 8 * b + 8, :]
        acc_re[b] = acc_re[b] + (amp_re * cosine + amp_im * sine)
        acc_im[b] = acc_im[b] + (amp_im * cosine - amp_re * sine)
        if b == 0:
            next_cos = cosine * step_cos - sine * step_sin
            next_sin = sine * step_cos + cosine * step_sin
        else:
            next_cos = twice * cosine - past_cos
            next_sin = twice * sine - past_sin
        past_cos, past_sin, cosine, sine = cosine, sine, next_cos, next_sin


def whole_kernel(
    share,
    flow_ref,
    weight_ref,
    owner_ref,
    block_ref,
    normal_ref,
    point_ref,
    observer_ref,
    table_ref,
    out_ref,
    slices,
    flows,
    weights,
    facts,
    onehot,
    outgoing,
    series_ref,
    observers_ref,
    points,
    rights,
    cosines,
    sines,
    terms,
    shifted,
    lefts,
    acc_ref,
    sums,
    arrived,
    flow_send,
    flow_recv,
    weight_send,
    weight_recv,
    fact_send,
    fact_recv,
    view_send,
    view_recv,
    series_send,
    series_recv,
    term_send,
    term_recv,
):
    owners = flows.shape[0]
    held = flow_ref.shape[0]
    cells = flow_ref.shape[1]
    spread = observers_ref.shape[0]
    members = share * spread
    samples = NT // members
    width = NV * samples
    slots = weight_ref.shape[1] // cells
    me_panel = lax.axis_index("panel")
    me_obs = lax.axis_index("obs")
    sub = lax.rem(me_panel, share)
    base = me_panel - sub
    mine = me_obs * share + sub

    def member(distance):
        return {
            "panel": base + flip(sub, distance // spread, share),
            "obs": flip(me_obs, distance % spread if isinstance(distance, int) else lax.rem(distance, spread), spread),
        }

    orders = acc_ref.shape[0] // 2
    panels = point_ref.shape[1]
    groups = panels // GROUP
    rows_out = out_ref.shape[0]
    ahead = onehot.shape[0] == members
    barrier = pltpu.get_barrier_semaphore()
    for turn in range(spread):

        def greet(shift, carry):
            pl.semaphore_signal(
                barrier,
                inc=1,
                device_id={"panel": lax.rem(me_panel + shift, owners), "obs": lax.rem(me_obs + turn, spread)},
                device_id_type=MESH,
            )
            return carry

        lax.fori_loop(1 if turn == 0 else 0, owners, greet, 0)

    def prepare(*accs):
        quarters, squares, talls, middles = accs[0:4], accs[4:6], accs[6:8], accs[8:10]
        quarter = share * samples
        rows = lax.broadcasted_iota(jnp.int32, (quarter, NT), 0)
        columns = lax.broadcasted_iota(jnp.int32, (quarter, NT), 1)
        pick = hot(columns == rows + me_obs * quarter)
        for turn, (cell, var) in enumerate((cell, var) for cell in range(0, cells, 2) for var in range(NV)):
            span = slice(var * NT, (var + 1) * NT)
            right = jnp.concatenate([flow_ref[:, cell, span], flow_ref[:, cell + 1, span]], axis=0)
            piece = product(quarters[turn % 4], turn % 2, [pick], [right], True).astype(jnp.bfloat16)
            for side in range(2):
                for part in range(share):
                    row = (cell + side) * width + var * samples
                    slices[part, row : row + samples, :] = piece[
                        part * samples : (part + 1) * samples, side * held : (side + 1) * held
                    ]
        facts[0] = jnp.zeros(facts.shape[1:], jnp.float32)
        facts[0, 0:1, :] = owner_ref[...].astype(jnp.float32)
        facts[0, 1:2, :] = block_ref[...].astype(jnp.float32)
        facts[0, 2:5, :] = normal_ref[...]
        place = lax.broadcasted_iota(jnp.int32, (slots * cells, slots * cells), 0)
        goal = lax.broadcasted_iota(jnp.int32, (slots * cells, slots * cells), 1)
        turn = hot(lax.rem(place, cells) * slots + place // cells == goal)
        for unit in range(2):
            span = slice(unit * 256, (unit + 1) * 256)
            tiles = [weight_ref[:, :256], weight_ref[:, 256:]]
            weights[0, :, span] = product(squares[unit], unit, tiles, [turn[:256, span], turn[256:, span]]).astype(jnp.bfloat16)
        observers_ref[me_obs] = observer_ref[...]

        points[...] = jnp.zeros_like(points)
        points[0:3, :] = point_ref[...]
        points[...] = jnp.transpose(points[...])

        pl.semaphore_wait(barrier, owners * spread - 1)

        def flow_copy(shift):
            target = flip(me_panel, shift, owners)
            return pltpu.make_async_remote_copy(
                src_ref=slices.at[lax.rem(target, share)],
                dst_ref=flows.at[me_panel],
                send_sem=flow_send.at[shift],
                recv_sem=flow_recv.at[shift],
                device_id={"panel": target},
                device_id_type=MESH,
            )

        def push(turn, carry):
            flow_copy(owners - turn).start()
            return carry

        def relay(buffer, send_sem, recv_sem, held_slot, bit):
            return pltpu.make_async_remote_copy(
                src_ref=buffer.at[held_slot],
                dst_ref=buffer.at[held_slot + bit],
                send_sem=send_sem.at[held_slot + bit],
                recv_sem=recv_sem.at[held_slot + bit],
                device_id=member(bit),
                device_id_type=MESH,
            )

        copies = {}

        def forward(slot):
            inner = slot % spread
            lowest = inner & -inner if inner else spread
            steps = [part * spread for part in range(1, share)] if slot == 0 else []
            bit = spread // 2
            while bit >= 1:
                steps.append(bit)
                bit //= 2
            for bit in steps:
                if bit < lowest or bit >= spread:
                    for kind, (buffer, send_sem, recv_sem) in enumerate(
                        ((facts, fact_send, fact_recv), (weights, weight_send, weight_recv))
                    ):
                        copy = relay(buffer, send_sem, recv_sem, slot, bit)
                        copy.start()
                        copies[kind, slot + bit] = copy

        forward(0)
        lax.fori_loop(1, owners, push, 0)

        def view_copy(shift):
            return pltpu.make_async_remote_copy(
                src_ref=observer_ref,
                dst_ref=observers_ref.at[me_obs],
                send_sem=view_send.at[shift],
                recv_sem=view_recv.at[shift],
                device_id={"obs": lax.rem(me_obs + shift, spread)},
                device_id_type=MESH,
            )

        views = [view_copy(shift) for shift in range(1, spread)]
        for view in views:
            view.start()
        flows[me_panel] = slices[sub]

        def survey(step):
            observers = observers_ref[lax.rem(me_obs + step + 1, spread)]

            @pl.loop(0, groups)
            def _(group):
                place = step * groups + group
                near = points[pl.ds(pl.multiple_of(group * GROUP, GROUP), GROUP), :]
                geometry(near, observers, rights.at[place], cosines.at[place], sines.at[place])

        def receive(slots_now):
            for slot in slots_now:
                copies[0, slot].wait_recv()
                copies[1, slot].wait_recv()
                forward(slot)

        order = sorted(
            range(1, members),
            key=lambda slot: (bin(slot % spread).count("1"), -(slot % spread), bin(slot).count("1"), -slot),
        )
        direct = share - 1
        survey(spread - 1)
        receive(order[:direct])
        for view in views:
            view.wait()
        for step in range(spread - 1):
            if step == 1:
                receive(order[direct : direct + share])
            survey(step)
        receive(order[direct + share :])

        names = lax.broadcasted_iota(jnp.int32, (held, slots), 0).astype(jnp.float32)

        def mark(slot, side):
            owner_row = facts[slot, 0:1, :]
            block_row = facts[slot, 1:2, :]

            def mark_owner(owner, inner):
                row = jnp.where(owner_row == owner.astype(jnp.float32), block_row, -1.0)
                onehot[side, pl.ds(pl.multiple_of(owner * held, held), held), :] = hot(names == row)
                return inner

            lax.fori_loop(0, owners, mark_owner, 0)

        if ahead:

            @pl.loop(0, members)
            def _(slot):
                mark(slot, slot)

        def drain(shift, carry):
            flow_copy(shift).wait()
            return carry

        lax.fori_loop(1, owners, drain, 0)

        chunk = min(owners, 8)

        def gathered(low, high):
            if not ahead:
                mark(low, 0)
                mark(high, 1)
            sides = (low, high) if ahead else (0, 1)

            def partial_of(start):
                terms_of = []
                for unit in range(2):
                    some = range(unit * chunk // 2, (unit + 1) * chunk // 2, 2)
                    left = [jnp.concatenate([flows[start + i], flows[start + i + 1]], axis=1) for i in some]
                    right = []
                    for i in some:
                        row = pl.ds(pl.multiple_of((start + i) * held, held), 2 * held)
                        right.append(jnp.concatenate([onehot[sides[0], row, :], onehot[sides[1], row, :]], axis=1))
                    terms_of.append(product(talls[unit], unit, left, right))
                return terms_of[0] + terms_of[1]

            total = partial_of(0)
            if owners > chunk:
                total = lax.fori_loop(1, owners // chunk, lambda i, run: run + partial_of(i * chunk), total)
            return total.astype(jnp.bfloat16)

        def values_of(low, high, donors):
            terms_of = []
            for unit in range(2):
                pairs = range(unit * cells // 2, (unit + 1) * cells // 2)
                left = []
                for side in range(2):
                    lanes = slice(side * slots, (side + 1) * slots)
                    left.append(jnp.concatenate([donors[cell * width : (cell + 1) * width, lanes] for cell in pairs], axis=1))
                span = slice(unit * 256, (unit + 1) * 256)
                right = jnp.concatenate([weights[low, :, span], weights[high, :, span]], axis=0)
                terms_of.append(product(middles[unit], unit, [jnp.concatenate(left, axis=0)], [right], True))
            both = terms_of[0] + terms_of[1]
            return both[:width, :panels], both[width:, panels:]

        def series_of(slot, values):
            field = [values[var * samples : (var + 1) * samples, :] for var in range(NV)]
            normal = [facts[slot, 2 + i : 3 + i, :] for i in range(3)]
            flow = field[1] * normal[0] + field[2] * normal[1] + field[3] * normal[2]
            mass = (1.0 + field[0]) * flow
            return [mass] + [field[4] * normal[i] + mass * field[1 + i] for i in range(3)]

        span = pl.ds(pl.multiple_of(mine * samples, samples), samples)

        def series_copy(slot):
            return pltpu.make_async_remote_copy(
                src_ref=outgoing.at[slot],
                dst_ref=series_ref.at[:, span, :],
                send_sem=series_send.at[slot],
                recv_sem=series_recv.at[slot],
                device_id=member(slot),
                device_id_type=MESH,
            )

        def finish(slot, values):
            for kind, term in enumerate(series_of(slot, values)):
                outgoing[slot, kind] = term
            series_copy(slot).start()


        def pair(step, carry):
            low = members - 2 * step
            high = low + 1
            first_values, second_values = values_of(low, high, gathered(low, high))
            finish(low, first_values)
            finish(high, second_values)
            return carry

        lax.fori_loop(1, members // 2, pair, 0)
        low_values, high_values = values_of(0, 1, gathered(0, 1))
        finish(1, high_values)
        for kind, term in enumerate(series_of(0, low_values)):
            series_ref[kind, span, :] = term

        for slot in range(1, members):
            copies[0, slot].wait_send()
            copies[1, slot].wait_send()

        def settle_series(slot, carry):
            series_copy(slot).wait()
            return carry

        lax.fori_loop(1, members, settle_series, 0)

        wavenum = KAPPA * (1 + lax.broadcasted_iota(jnp.int32, (orders, panels), 0)).astype(jnp.float32)
        for unit in range(2):
            rest = jnp.concatenate([series_ref[2 * unit], series_ref[2 * unit + 1]], axis=1)
            left, right = [], []
            for depth in range(3):
                part = rest.astype(jnp.bfloat16)
                rest = rest - part.astype(jnp.float32)
                for level in range(3 - depth):
                    left.append(table_ref[level])
                    right.append(part)
            both = product(squares[unit], unit, left, right)
            for side in range(2):
                kind = 2 * unit + side
                near = both[:, side * panels : (side + 1) * panels]
                far = jnp.concatenate([-wavenum * near[orders:], wavenum * near[:orders]], axis=0)
                if kind == 0:
                    terms[6] = far
                else:
                    terms[kind - 1] = near
                    terms[kind + 2] = far
        lane = lax.broadcasted_iota(jnp.int32, (1, panels), 1)

        for slot in range(SLOT - 1):
            high, low = split_hi_lo(terms[slot])
            shifted[slot] = pltpu.roll(high, slot * GROUP, 1) if slot else high
            shifted[SLOT + slot] = pltpu.roll(low, (SLOT + slot) * GROUP, 1)

        @pl.loop(0, groups)
        def _(group):
            kind = lax.rem(lane // GROUP + (groups - group), groups)
            both = jnp.zeros((2 * orders, panels), jnp.float32)
            for slot in range(SLOT - 1):
                both = jnp.where(kind == slot, shifted[slot], both)
                both = jnp.where(kind == SLOT + slot, shifted[SLOT + slot], both)
            moved = pltpu.roll(both, lax.rem((groups - group) * GROUP, panels), 1)
            lefts[group] = moved.astype(jnp.bfloat16)

    def term_copy(step, shift):
        slot = lax.rem(step + 1, spread) * owners + shift
        target = lax.rem(me_panel + shift, owners)
        return pltpu.make_async_remote_copy(
            src_ref=sums.at[step, target],
            dst_ref=arrived.at[slot],
            send_sem=term_send.at[slot],
            recv_sem=term_recv.at[slot],
            device_id={"panel": target, "obs": lax.rem(me_obs + step + 1, spread)},
            device_id_type=MESH,
        )

    def radiate(*accs):

        last = spread * groups - 1
        load_right(rights.at[0])
        for y in range(GROUP):
            amplitude(accs[y], y, lefts[0], y < 2)
        load_right(rights.at[1])

        @pl.loop(0, spread)
        def _(step):
            acc_ref[...] = jnp.zeros_like(acc_ref)

            @pl.loop(0, groups)
            def _(group):
                place = step * groups + group
                after = jnp.minimum(place + 1, last)
                left = lefts[lax.rem(after, groups)]
                blocks = orders // 8
                acc_re = [acc_ref[pl.ds(8 * b, 8), :] for b in range(blocks)]
                acc_im = [acc_ref[pl.ds(orders + 8 * b, 8), :] for b in range(blocks)]
                for y in range(GROUP):
                    amp = pltpu.matmul_pop(accs[y])
                    amplitude(accs[y], y, left, y < 2)
                    if y == 1:
                        load_right(rights.at[jnp.minimum(place + 2, last)])
                    steps = (cosines[place, y, 7:8, :], sines[place, y, 7:8, :])
                    accumulate(amp, cosines[place, y], sines[place, y], *steps, acc_re, acc_im)
                for b in range(blocks):
                    acc_ref[pl.ds(8 * b, 8), :] = acc_re[b]
                    acc_ref[pl.ds(orders + 8 * b, 8), :] = acc_im[b]

            for owner in range(owners):
                sums[step, owner] = acc_ref[owner * rows_out : (owner + 1) * rows_out, :]

            @pl.when(step < spread - 1)
            def _():
                term_copy(step, 0).start()

            def push(shift, carry):
                term_copy(step, shift).start()
                return carry

            lax.fori_loop(1, owners, push, 0)

        for y in range(2):
            amplitude(accs[y], y, lefts[0], True)
        for acc in accs:
            pltpu.matmul_pop(acc)

    def store(unit, height):
        return pltpu.ACC(unit)((height, 256), jnp.float32)

    part_rows = share * samples
    pl.run_scoped(
        prepare,
        *[store(turn % 2, part_rows) for turn in range(4)],
        *[store(unit, 2 * orders) for unit in range(2)],
        *[store(unit, cells * width) for unit in range(2)],
        *[store(unit, 2 * width) for unit in range(2)],
    )
    pl.run_scoped(radiate, *[store(y % 2, 2 * orders) for y in range(GROUP)])

    arrived[0] = sums[spread - 1, me_panel]
    for step in range(spread):

        def settle(shift, carry):
            term_copy(step, shift).wait()
            return carry

        lax.fori_loop(1 if step == spread - 1 else 0, owners, settle, 0)

    def add(slot, total):
        return total + arrived[slot]

    out_ref[...] = lax.fori_loop(1, owners * spread, add, arrived[0])


def run(flow, weight, owner, block, normals, points, observers):
    owners = lax.axis_size("panel")
    spread = lax.axis_size("obs")
    share = max(1, min(owners, 16 // spread))
    members = share * spread
    held, cells, history = flow.shape
    panels = normals.shape[1]
    count = observers.shape[1]
    samples = NT // members
    width = NV * samples
    slots = weight.shape[1] // cells
    places = spread * (panels // GROUP)
    rows = 2 * HARM // owners
    ahead = members * owners * held * slots <= 1 << 22
    bf16, f32 = jnp.bfloat16, jnp.float32
    vmem = pl.BlockSpec(memory_space=pltpu.VMEM)
    dma = pltpu.SemaphoreType.DMA
    wave = pltpu.VMEM((places, GROUP, 8, count), f32)
    return pl.pallas_call(
        functools.partial(whole_kernel, share),
        out_shape=jax.ShapeDtypeStruct((rows, count), f32),
        in_specs=[vmem] * 8,
        out_specs=vmem,
        scratch_shapes=[
            pltpu.VMEM((share, cells * width, held), bf16),
            pltpu.VMEM((owners, cells * width, held), bf16),
            pltpu.VMEM((members,) + weight.shape, bf16),
            pltpu.VMEM((members, 8, panels), f32),
            pltpu.VMEM((members if ahead else 2, owners * held, slots), bf16),
            pltpu.VMEM((members, SERIES, samples, panels), f32),
            pltpu.VMEM((SERIES, NT, panels), f32),
            pltpu.VMEM((spread,) + observers.shape, f32),
            pltpu.VMEM((panels, panels), f32),
            pltpu.VMEM((places, 2 * SLOT * GROUP, count), bf16),
            wave,
            wave,
            pltpu.VMEM((SLOT - 1, 2 * HARM, panels), f32),
            pltpu.VMEM((2 * SLOT, 2 * HARM, panels), f32),
            pltpu.VMEM((panels // GROUP, 2 * HARM, panels), bf16),
            pltpu.VMEM((2 * HARM, count), f32),
            pltpu.VMEM((spread, owners, rows, count), f32),
            pltpu.VMEM((spread * owners, rows, count), f32),
            dma((owners,)),
            dma((owners,)),
            dma((members,)),
            dma((members,)),
            dma((members,)),
            dma((members,)),
            dma((spread,)),
            dma((spread,)),
            dma((members,)),
            dma((members,)),
            dma((spread * owners,)),
            dma((spread * owners,)),
        ],
        compiler_params=pltpu.CompilerParams(
            collective_id=1,
            has_side_effects=True,
            vmem_limit_bytes=63000 * 1024,
        ),
        name="whole",
    )(flow, weight, owner, block, normals, points, observers, jnp.asarray(three_parts(fourier_rows(NT, HARM))))


def body(
    flow_blocks,
    interp_weights,
    donor_owner,
    donor_block,
    panel_normals,
    panel_points,
    observer_points,
):
    tiles, width, stencil = interp_weights.shape
    return run(
        flow_blocks,
        interp_weights.reshape(tiles * width, stencil),
        donor_owner.reshape(1, -1),
        donor_block.reshape(1, -1),
        panel_normals,
        panel_points,
        observer_points,
    )


def solution(mesh):
    return jax.shard_map(
        body,
        mesh=mesh,
        in_specs=(
            P("panel", None, None),
            P(("panel", "obs"), None, None),
            P(("panel", "obs"), None),
            P(("panel", "obs")),
            P(None, ("panel", "obs")),
            P(None, ("panel", "obs")),
            P(None, "obs"),
        ),
        out_specs=P("panel", "obs"),
        check_vma=False,
    )
```

```python
import functools
import math

import jax
import jax.numpy as jnp
import numpy as np
from jax import lax
from jax.experimental import pallas as pl
from jax.experimental.pallas import tpu as pltpu
from jax.sharding import PartitionSpec as P

NV = 5
NT = 256
HARM = 64
SERIES = 4
GROUP = 8
SLOT = 8
KAPPA = 0.5
MESH = pl.DeviceIdType.MESH


def fourier_rows(samples, orders):
    wrapped = np.arange(1, orders + 1)[:, None] * np.arange(samples)[None, :] % samples
    angles = wrapped * (2.0 * np.pi / samples)
    factor = 2.0 / samples
    return np.concatenate([factor * np.cos(angles), -factor * np.sin(angles)], axis=0).astype(np.float32)


def three_parts(table):
    parts = []
    rest = table.astype(np.float64)
    for _ in range(3):
        part = rest.astype(jnp.bfloat16)
        parts.append(part)
        rest = rest - part.astype(np.float64)
    return np.stack(parts)


def flip(index, bits, width):
    out = index
    bit = 1
    while bit < width:
        mine = lax.rem(index // bit, 2) if not isinstance(index, int) else (index // bit) % 2
        theirs = lax.rem(bits // bit, 2) if not isinstance(bits, int) else (bits // bit) % 2
        if not isinstance(bits, int) or theirs:
            out = out + bit * theirs * (1 - 2 * mine)
        bit *= 2
    return out


def hot(condition):
    return jnp.where(condition, 1.0, 0.0).astype(jnp.bfloat16)


def product(acc, unit, lefts, rights, transpose=False):
    for turn, (left, right) in enumerate(zip(lefts, rights)):
        pltpu.matmul_push_rhs(right, staging_register=turn % 2, mxu_index=unit, transpose=transpose)
        pltpu.matmul_acc_lhs(acc, left, load_staged_rhs=turn % 2)
    return pltpu.matmul_pop(acc)


def sin_cos(angle):
    turns = jnp.floor(angle * (2.0 / math.pi) + 0.5)
    reduced = angle - turns * 1.5703125
    reduced = reduced - turns * 4.837512969970703125e-4
    reduced = reduced - turns * 7.54978995489188216e-8
    square = reduced * reduced
    sine = ((-1.9515295891e-4 * square + 8.3321608736e-3) * square - 1.6666654611e-1) * square * reduced + reduced
    cosine = ((2.443315711809948e-5 * square - 1.388731625493765e-3) * square + 4.166664568298827e-2) * square * square - 0.5 * square + 1.0
    quadrant = turns.astype(jnp.int32)
    swap = (quadrant & 1) == 1
    out_sin = jnp.where(swap, cosine, sine)
    out_cos = jnp.where(swap, sine, cosine)
    out_sin = jnp.where((quadrant & 2) == 2, -out_sin, out_sin)
    out_cos = jnp.where(((quadrant + 1) & 2) == 2, -out_cos, out_cos)
    return out_sin, out_cos


def split_hi_lo(array):
    high = array.astype(jnp.bfloat16).astype(jnp.float32)
    return high, array - high


def geometry(points, observers, right_ref, cos_ref, sin_ref):
    offsets = [observers[i : i + 1, :] - points[:, i : i + 1] for i in range(3)]
    squared = offsets[0] * offsets[0] + offsets[1] * offsets[1] + offsets[2] * offsets[2]
    distance = jnp.sqrt(squared)
    inverse = 1.0 / distance
    weight = inverse * (1.0 / (4.0 * math.pi))
    far = [offset * (inverse * weight) for offset in offsets]
    near = [term * inverse for term in far]
    slots = near + far + [weight, jnp.zeros_like(weight)]
    high, low = split_hi_lo(jnp.concatenate(slots, axis=0))
    right_ref[...] = jnp.concatenate([high, low], axis=0).astype(jnp.bfloat16)
    sine, cosine = sin_cos(KAPPA * distance)
    twice = 2.0 * cosine
    past_cos, past_sin = jnp.ones_like(cosine), jnp.zeros_like(sine)
    for order in range(8):
        cos_ref[:, order, :] = cosine
        sin_ref[:, order, :] = sine
        cosine, past_cos = twice * cosine - past_cos, cosine
        sine, past_sin = twice * sine - past_sin, sine


def load_right(right_ref):
    half = right_ref.shape[0] // 2
    high, low = right_ref[:half, :], right_ref[half:, :]
    right = jnp.concatenate([high, high, low, low], axis=0)
    for unit in range(2):
        pltpu.matmul_push_rhs(right, staging_register=0, mxu_index=unit)


def amplitude(acc, y, left, fresh):
    lanes = lax.rem(lax.broadcasted_iota(jnp.int32, (1, left.shape[1]), 1), GROUP)
    one = left * (lanes == y).astype(jnp.float32).astype(jnp.bfloat16)
    both = jnp.concatenate([one, one], axis=1)
    pltpu.matmul_acc_lhs(acc, both, load_staged_rhs=0 if fresh else None)


def accumulate(amp, cosine, sine, step_cos, step_sin, acc_re, acc_im):
    blocks = len(acc_re)
    orders = amp.shape[0] // 2
    twice = 2.0 * step_cos
    past_cos = past_sin = None
    for b in range(blocks):
        amp_re = amp[8 * b : 8 * b + 8, :]
        amp_im = amp[orders + 8 * b : orders + 8 * b + 8, :]
        acc_re[b] = acc_re[b] + (amp_re * cosine + amp_im * sine)
        acc_im[b] = acc_im[b] + (amp_im * cosine - amp_re * sine)
        if b == 0:
            next_cos = cosine * step_cos - sine * step_sin
            next_sin = sine * step_cos + cosine * step_sin
        else:
            next_cos = twice * cosine - past_cos
            next_sin = twice * sine - past_sin
        past_cos, past_sin, cosine, sine = cosine, sine, next_cos, next_sin


def whole_kernel(
    share,
    flow_hbm,
    weight_ref,
    owner_ref,
    block_ref,
    normal_ref,
    point_ref,
    observer_ref,
    table_ref,
    out_ref,
    flow_ref,
    slices,
    flows,
    weights,
    facts,
    onehot,
    outgoing,
    series_ref,
    observers_ref,
    points,
    rights,
    cosines,
    sines,
    terms,
    shifted,
    lefts,
    acc_ref,
    sums,
    arrived,
    flow_send,
    flow_recv,
    weight_send,
    weight_recv,
    fact_send,
    fact_recv,
    view_send,
    view_recv,
    series_send,
    series_recv,
    term_send,
    term_recv,
    flow_load,
):
    owners = flows.shape[0]
    held = flow_ref.shape[0]
    cells = flow_ref.shape[1]
    spread = observers_ref.shape[0]
    members = share * spread
    samples = NT // members
    width = NV * samples
    slots = weight_ref.shape[1] // cells
    me_panel = lax.axis_index("panel")
    me_obs = lax.axis_index("obs")
    sub = lax.rem(me_panel, share)
    base = me_panel - sub
    mine = me_obs * share + sub

    def member(distance):
        return {
            "panel": base + flip(sub, distance // spread, share),
            "obs": flip(me_obs, distance % spread if isinstance(distance, int) else lax.rem(distance, spread), spread),
        }

    orders = acc_ref.shape[0] // 2
    panels = point_ref.shape[1]
    groups = panels // GROUP
    rows_out = out_ref.shape[0]
    ahead = onehot.shape[0] == members
    load = pltpu.make_async_copy(flow_hbm, flow_ref, flow_load)
    load.start()
    barrier = pltpu.get_barrier_semaphore()
    for turn in range(spread):

        def greet(shift, carry):
            pl.semaphore_signal(
                barrier,
                inc=1,
                device_id={"panel": lax.rem(me_panel + shift, owners), "obs": lax.rem(me_obs + turn, spread)},
                device_id_type=MESH,
            )
            return carry

        lax.fori_loop(1 if turn == 0 else 0, owners, greet, 0)

    def prepare(*accs):
        quarters, squares, talls, middles = accs[0:4], accs[4:6], accs[6:8], accs[8:10]
        facts[0] = jnp.zeros(facts.shape[1:], jnp.float32)
        facts[0, 0:1, :] = owner_ref[...].astype(jnp.float32)
        facts[0, 1:2, :] = block_ref[...].astype(jnp.float32)
        facts[0, 2:5, :] = normal_ref[...]
        place = lax.broadcasted_iota(jnp.int32, (slots * cells, slots * cells), 0)
        goal = lax.broadcasted_iota(jnp.int32, (slots * cells, slots * cells), 1)
        turn = hot(lax.rem(place, cells) * slots + place // cells == goal)
        for unit in range(2):
            span = slice(unit * 256, (unit + 1) * 256)
            tiles = [weight_ref[:, :256], weight_ref[:, 256:]]
            weights[0, :, span] = product(squares[unit], unit, tiles, [turn[:256, span], turn[256:, span]]).astype(jnp.bfloat16)
        observers_ref[me_obs] = observer_ref[...]

        points[...] = jnp.zeros_like(points)
        points[0:3, :] = point_ref[...]
        points[...] = jnp.transpose(points[...])

        pl.semaphore_wait(barrier, owners * spread - 1)

        def flow_copy(shift):
            target = flip(me_panel, shift, owners)
            return pltpu.make_async_remote_copy(
                src_ref=slices.at[lax.rem(target, share)],
                dst_ref=flows.at[me_panel],
                send_sem=flow_send.at[shift],
                recv_sem=flow_recv.at[shift],
                device_id={"panel": target},
                device_id_type=MESH,
            )

        def push(turn, carry):
            flow_copy(owners - turn).start()
            return carry

        def relay(buffer, send_sem, recv_sem, held_slot, bit):
            return pltpu.make_async_remote_copy(
                src_ref=buffer.at[held_slot],
                dst_ref=buffer.at[held_slot + bit],
                send_sem=send_sem.at[held_slot + bit],
                recv_sem=recv_sem.at[held_slot + bit],
                device_id=member(bit),
                device_id_type=MESH,
            )

        copies = {}

        def forward(slot):
            inner = slot % spread
            lowest = inner & -inner if inner else spread
            steps = [part * spread for part in range(1, share)] if slot == 0 else []
            bit = spread // 2
            while bit >= 1:
                steps.append(bit)
                bit //= 2
            for bit in steps:
                if bit < lowest or bit >= spread:
                    for kind, (buffer, send_sem, recv_sem) in enumerate(
                        ((facts, fact_send, fact_recv), (weights, weight_send, weight_recv))
                    ):
                        copy = relay(buffer, send_sem, recv_sem, slot, bit)
                        copy.start()
                        copies[kind, slot + bit] = copy

        forward(0)

        quarter = share * samples
        rows = lax.broadcasted_iota(jnp.int32, (2 * quarter, 256), 0)
        columns = lax.broadcasted_iota(jnp.int32, (2 * quarter, 256), 1)
        shift = lax.rem(me_obs * quarter, 128)
        tile = pl.multiple_of(me_obs * quarter - shift, 128)
        pick = hot((columns // 128 == rows // quarter) & (lax.rem(columns, 128) == lax.rem(rows, quarter) + shift))
        load.wait()
        for turn, (cell, var) in enumerate((cell, var) for cell in range(0, cells, 2) for var in range(0, NV, 2)):
            halves = [var, min(var + 1, NV - 1)]
            right = jnp.concatenate(
                [
                    jnp.concatenate([flow_ref[:, cell + side, pl.ds(one * NT + tile, 128)] for one in halves], axis=1)
                    for side in range(2)
                ],
                axis=0,
            )
            piece = product(quarters[turn % 4], turn % 2, [pick], [right], True).astype(jnp.bfloat16)
            for half in range(len(set(halves))):
                for side in range(2):
                    for part in range(share):
                        row = (cell + side) * width + (var + half) * samples
                        start = half * quarter + part * samples
                        slices[part, row : row + samples, :] = piece[
                            start : start + samples, side * held : (side + 1) * held
                        ]

        lax.fori_loop(1, owners, push, 0)

        def view_copy(shift):
            return pltpu.make_async_remote_copy(
                src_ref=observer_ref,
                dst_ref=observers_ref.at[me_obs],
                send_sem=view_send.at[shift],
                recv_sem=view_recv.at[shift],
                device_id={"obs": lax.rem(me_obs + shift, spread)},
                device_id_type=MESH,
            )

        views = [view_copy(shift) for shift in range(1, spread)]
        for view in views:
            view.start()
        flows[me_panel] = slices[sub]

        def survey(step):
            observers = observers_ref[lax.rem(me_obs + step + 1, spread)]

            @pl.loop(0, groups)
            def _(group):
                place = step * groups + group
                near = points[pl.ds(pl.multiple_of(group * GROUP, GROUP), GROUP), :]
                geometry(near, observers, rights.at[place], cosines.at[place], sines.at[place])

        def receive(slots_now):
            for slot in slots_now:
                copies[0, slot].wait_recv()
                copies[1, slot].wait_recv()
                forward(slot)

        order = sorted(
            range(1, members),
            key=lambda slot: (bin(slot % spread).count("1"), -(slot % spread), bin(slot).count("1"), -slot),
        )
        direct = share - 1
        survey(spread - 1)
        receive(order[:direct])
        for view in views:
            view.wait()
        for step in range(spread - 1):
            if step == 2:
                receive(order[direct : direct + share])
            survey(step)
        ends = order[direct + share :]
        for slot in ends:
            copies[0, slot].wait_recv()

        names = lax.broadcasted_iota(jnp.int32, (held, slots), 0).astype(jnp.float32)

        def mark(slot, side):
            owner_row = facts[slot, 0:1, :]
            block_row = facts[slot, 1:2, :]

            def mark_owner(owner, inner):
                row = jnp.where(owner_row == owner.astype(jnp.float32), block_row, -1.0)
                onehot[side, pl.ds(pl.multiple_of(owner * held, held), held), :] = hot(names == row)
                return inner

            lax.fori_loop(0, owners, mark_owner, 0)

        if ahead:

            @pl.loop(0, members)
            def _(slot):
                mark(slot, slot)

        def drain(shift, carry):
            flow_copy(shift).wait()
            return carry

        lax.fori_loop(1, owners, drain, 0)
        for slot in ends:
            copies[1, slot].wait_recv()

        chunk = min(owners, 8)

        def gathered(low, high):
            if not ahead:
                mark(low, 0)
                mark(high, 1)
            sides = (low, high) if ahead else (0, 1)

            def partial_of(start):
                terms_of = []
                for unit in range(2):
                    some = range(unit * chunk // 2, (unit + 1) * chunk // 2, 2)
                    left = [jnp.concatenate([flows[start + i], flows[start + i + 1]], axis=1) for i in some]
                    right = []
                    for i in some:
                        row = pl.ds(pl.multiple_of((start + i) * held, held), 2 * held)
                        right.append(jnp.concatenate([onehot[sides[0], row, :], onehot[sides[1], row, :]], axis=1))
                    terms_of.append(product(talls[unit], unit, left, right))
                return terms_of[0] + terms_of[1]

            total = partial_of(0)
            if owners > chunk:
                total = lax.fori_loop(1, owners // chunk, lambda i, run: run + partial_of(i * chunk), total)
            return total.astype(jnp.bfloat16)

        def values_of(low, high, donors):
            terms_of = []
            for unit in range(2):
                pairs = range(unit * cells // 2, (unit + 1) * cells // 2)
                left = []
                for side in range(2):
                    lanes = slice(side * slots, (side + 1) * slots)
                    left.append(jnp.concatenate([donors[cell * width : (cell + 1) * width, lanes] for cell in pairs], axis=1))
                span = slice(unit * 256, (unit + 1) * 256)
                right = jnp.concatenate([weights[low, :, span], weights[high, :, span]], axis=0)
                terms_of.append(product(middles[unit], unit, [jnp.concatenate(left, axis=0)], [right], True))
            both = terms_of[0] + terms_of[1]
            return both[:width, :panels], both[width:, panels:]

        def series_of(slot, values):
            field = [values[var * samples : (var + 1) * samples, :] for var in range(NV)]
            normal = [facts[slot, 2 + i : 3 + i, :] for i in range(3)]
            flow = field[1] * normal[0] + field[2] * normal[1] + field[3] * normal[2]
            mass = (1.0 + field[0]) * flow
            return [mass] + [field[4] * normal[i] + mass * field[1 + i] for i in range(3)]

        span = pl.ds(pl.multiple_of(mine * samples, samples), samples)

        def series_copy(slot):
            return pltpu.make_async_remote_copy(
                src_ref=outgoing.at[slot],
                dst_ref=series_ref.at[:, span, :],
                send_sem=series_send.at[slot],
                recv_sem=series_recv.at[slot],
                device_id=member(slot),
                device_id_type=MESH,
            )

        def finish(slot, values):
            for kind, term in enumerate(series_of(slot, values)):
                outgoing[slot, kind] = term
            series_copy(slot).start()


        def pair(step, donors):
            low = members - 2 * step
            high = low + 1
            following = gathered(low - 2, high - 2)
            first_values, second_values = values_of(low, high, donors)
            finish(low, first_values)
            finish(high, second_values)
            return following

        donors = lax.fori_loop(1, members // 2, pair, gathered(members - 2, members - 1))
        low_values, high_values = values_of(0, 1, donors)
        finish(1, high_values)
        for kind, term in enumerate(series_of(0, low_values)):
            series_ref[kind, span, :] = term

        for slot in range(1, members):
            copies[0, slot].wait_send()
            copies[1, slot].wait_send()

        def settle_series(slot, carry):
            series_copy(slot).wait()
            return carry

        lax.fori_loop(1, members, settle_series, 0)

        wavenum = KAPPA * (1 + lax.broadcasted_iota(jnp.int32, (orders, panels), 0)).astype(jnp.float32)
        for unit in range(2):
            rest = jnp.concatenate([series_ref[2 * unit], series_ref[2 * unit + 1]], axis=1)
            left, right = [], []
            for depth in range(3):
                part = rest.astype(jnp.bfloat16)
                rest = rest - part.astype(jnp.float32)
                for level in range(3 - depth):
                    left.append(table_ref[level])
                    right.append(part)
            both = product(squares[unit], unit, left, right)
            for side in range(2):
                kind = 2 * unit + side
                near = both[:, side * panels : (side + 1) * panels]
                far = jnp.concatenate([-wavenum * near[orders:], wavenum * near[:orders]], axis=0)
                if kind == 0:
                    terms[6] = far
                else:
                    terms[kind - 1] = near
                    terms[kind + 2] = far
        lane = lax.broadcasted_iota(jnp.int32, (1, panels), 1)

        for slot in range(SLOT - 1):
            high, low = split_hi_lo(terms[slot])
            shifted[slot] = pltpu.roll(high, slot * GROUP, 1) if slot else high
            shifted[SLOT + slot] = pltpu.roll(low, (SLOT + slot) * GROUP, 1)

        @pl.loop(0, groups)
        def _(group):
            kind = lax.rem(lane // GROUP + (groups - group), groups)
            both = jnp.zeros((2 * orders, panels), jnp.float32)
            for slot in range(SLOT - 1):
                both = jnp.where(kind == slot, shifted[slot], both)
                both = jnp.where(kind == SLOT + slot, shifted[SLOT + slot], both)
            moved = pltpu.roll(both, lax.rem((groups - group) * GROUP, panels), 1)
            lefts[group] = moved.astype(jnp.bfloat16)

    def term_copy(step, shift):
        slot = lax.rem(step + 1, spread) * owners + shift
        target = lax.rem(me_panel + shift, owners)
        return pltpu.make_async_remote_copy(
            src_ref=sums.at[step, target],
            dst_ref=arrived.at[slot],
            send_sem=term_send.at[slot],
            recv_sem=term_recv.at[slot],
            device_id={"panel": target, "obs": lax.rem(me_obs + step + 1, spread)},
            device_id_type=MESH,
        )

    def radiate(*accs):

        last = spread * groups - 1
        load_right(rights.at[0])
        for y in range(GROUP):
            amplitude(accs[y], y, lefts[0], y < 2)
        load_right(rights.at[1])

        @pl.loop(0, spread)
        def _(step):
            acc_ref[...] = jnp.zeros_like(acc_ref)

            @pl.loop(0, groups)
            def _(group):
                place = step * groups + group
                after = jnp.minimum(place + 1, last)
                left = lefts[lax.rem(after, groups)]
                blocks = orders // 8
                acc_re = [acc_ref[pl.ds(8 * b, 8), :] for b in range(blocks)]
                acc_im = [acc_ref[pl.ds(orders + 8 * b, 8), :] for b in range(blocks)]
                for y in range(GROUP):
                    amp = pltpu.matmul_pop(accs[y])
                    amplitude(accs[y], y, left, y < 2)
                    if y == 1:
                        load_right(rights.at[jnp.minimum(place + 2, last)])
                    steps = (cosines[place, y, 7:8, :], sines[place, y, 7:8, :])
                    accumulate(amp, cosines[place, y], sines[place, y], *steps, acc_re, acc_im)
                for b in range(blocks):
                    acc_ref[pl.ds(8 * b, 8), :] = acc_re[b]
                    acc_ref[pl.ds(orders + 8 * b, 8), :] = acc_im[b]

            for owner in range(owners):
                sums[step, owner] = acc_ref[owner * rows_out : (owner + 1) * rows_out, :]

            @pl.when(step < spread - 1)
            def _():
                term_copy(step, 0).start()

            def push(shift, carry):
                term_copy(step, shift).start()
                return carry

            lax.fori_loop(1, owners, push, 0)

        for y in range(2):
            amplitude(accs[y], y, lefts[0], True)
        for acc in accs:
            pltpu.matmul_pop(acc)

    def store(unit, height):
        return pltpu.ACC(unit)((height, 256), jnp.float32)

    part_rows = share * samples
    pl.run_scoped(
        prepare,
        *[store(turn % 2, 2 * part_rows) for turn in range(4)],
        *[store(unit, 2 * orders) for unit in range(2)],
        *[store(unit, cells * width) for unit in range(2)],
        *[store(unit, 2 * width) for unit in range(2)],
    )
    pl.run_scoped(radiate, *[store(y % 2, 2 * orders) for y in range(GROUP)])

    def settle(step):
        def one(shift, carry):
            term_copy(step, shift).wait()
            return carry

        lax.fori_loop(1 if step == spread - 1 else 0, owners, one, 0)

    def add(slot, total):
        return total + arrived[slot]

    for step in range(spread - 1):
        settle(step)
    early = lax.fori_loop(owners, owners * spread, add, sums[spread - 1, me_panel])
    settle(spread - 1)
    if owners <= 8:
        for slot in range(1, owners):
            early = early + arrived[slot]
    else:
        early = lax.fori_loop(1, owners, add, early)
    out_ref[...] = early


def run(flow, weight, owner, block, normals, points, observers):
    owners = lax.axis_size("panel")
    spread = lax.axis_size("obs")
    share = max(1, min(owners, 16 // spread))
    members = share * spread
    held, cells, history = flow.shape
    panels = normals.shape[1]
    count = observers.shape[1]
    samples = NT // members
    width = NV * samples
    slots = weight.shape[1] // cells
    places = spread * (panels // GROUP)
    rows = 2 * HARM // owners
    ahead = members * owners * held * slots <= 1 << 22
    bf16, f32 = jnp.bfloat16, jnp.float32
    vmem = pl.BlockSpec(memory_space=pltpu.VMEM)
    dma = pltpu.SemaphoreType.DMA
    wave = pltpu.VMEM((places, GROUP, 8, count), f32)
    return pl.pallas_call(
        functools.partial(whole_kernel, share),
        out_shape=jax.ShapeDtypeStruct((rows, count), f32),
        in_specs=[pl.BlockSpec(memory_space=pl.ANY)] + [vmem] * 7,
        out_specs=vmem,
        scratch_shapes=[
            pltpu.VMEM(flow.shape, bf16),
            pltpu.VMEM((share, cells * width, held), bf16),
            pltpu.VMEM((owners, cells * width, held), bf16),
            pltpu.VMEM((members,) + weight.shape, bf16),
            pltpu.VMEM((members, 8, panels), f32),
            pltpu.VMEM((members if ahead else 2, owners * held, slots), bf16),
            pltpu.VMEM((members, SERIES, samples, panels), f32),
            pltpu.VMEM((SERIES, NT, panels), f32),
            pltpu.VMEM((spread,) + observers.shape, f32),
            pltpu.VMEM((panels, panels), f32),
            pltpu.VMEM((places, 2 * SLOT * GROUP, count), bf16),
            wave,
            wave,
            pltpu.VMEM((SLOT - 1, 2 * HARM, panels), f32),
            pltpu.VMEM((2 * SLOT, 2 * HARM, panels), f32),
            pltpu.VMEM((panels // GROUP, 2 * HARM, panels), bf16),
            pltpu.VMEM((2 * HARM, count), f32),
            pltpu.VMEM((spread, owners, rows, count), f32),
            pltpu.VMEM((spread * owners, rows, count), f32),
            dma((owners,)),
            dma((owners,)),
            dma((members,)),
            dma((members,)),
            dma((members,)),
            dma((members,)),
            dma((spread,)),
            dma((spread,)),
            dma((members,)),
            dma((members,)),
            dma((spread * owners,)),
            dma((spread * owners,)),
            dma,
        ],
        compiler_params=pltpu.CompilerParams(
            collective_id=1,
            has_side_effects=True,
            vmem_limit_bytes=63000 * 1024,
        ),
        name="whole",
    )(flow, weight, owner, block, normals, points, observers, jnp.asarray(three_parts(fourier_rows(NT, HARM))))


def body(
    flow_blocks,
    interp_weights,
    donor_owner,
    donor_block,
    panel_normals,
    panel_points,
    observer_points,
):
    tiles, width, stencil = interp_weights.shape
    return run(
        flow_blocks,
        interp_weights.reshape(tiles * width, stencil),
        donor_owner.reshape(1, -1),
        donor_block.reshape(1, -1),
        panel_normals,
        panel_points,
        observer_points,
    )


def solution(mesh):
    return jax.shard_map(
        body,
        mesh=mesh,
        in_specs=(
            P("panel", None, None),
            P(("panel", "obs"), None, None),
            P(("panel", "obs"), None),
            P(("panel", "obs")),
            P(None, ("panel", "obs")),
            P(None, ("panel", "obs")),
            P(None, "obs"),
        ),
        out_specs=P("panel", "obs"),
        check_vma=False,
    )
```

```python
import functools
import math

import jax
import jax.numpy as jnp
import numpy as np
from jax import lax
from jax.experimental import pallas as pl
from jax.experimental.pallas import tpu as pltpu
from jax.sharding import PartitionSpec as P

NV = 5
NT = 256
HARM = 64
SERIES = 4
GROUP = 8
SLOT = 8
KAPPA = 0.5
MESH = pl.DeviceIdType.MESH


def fourier_rows(samples, orders):
    wrapped = np.arange(1, orders + 1)[:, None] * np.arange(samples)[None, :] % samples
    angles = wrapped * (2.0 * np.pi / samples)
    factor = 2.0 / samples
    return np.concatenate([factor * np.cos(angles), -factor * np.sin(angles)], axis=0).astype(np.float32)


def three_parts(table):
    parts = []
    rest = table.astype(np.float64)
    for _ in range(3):
        part = rest.astype(jnp.bfloat16)
        parts.append(part)
        rest = rest - part.astype(np.float64)
    return np.stack(parts)


def flip(index, bits, width):
    out = index
    bit = 1
    while bit < width:
        mine = lax.rem(index // bit, 2) if not isinstance(index, int) else (index // bit) % 2
        theirs = lax.rem(bits // bit, 2) if not isinstance(bits, int) else (bits // bit) % 2
        if not isinstance(bits, int) or theirs:
            out = out + bit * theirs * (1 - 2 * mine)
        bit *= 2
    return out


def hot(condition):
    return jnp.where(condition, 1.0, 0.0).astype(jnp.bfloat16)


def product(acc, unit, lefts, rights, transpose=False):
    for turn, (left, right) in enumerate(zip(lefts, rights)):
        pltpu.matmul_push_rhs(right, staging_register=turn % 2, mxu_index=unit, transpose=transpose)
        pltpu.matmul_acc_lhs(acc, left, load_staged_rhs=turn % 2)
    return pltpu.matmul_pop(acc)


def sin_cos(angle):
    turns = jnp.floor(angle * (2.0 / math.pi) + 0.5)
    reduced = angle - turns * 1.5703125
    reduced = reduced - turns * 4.837512969970703125e-4
    reduced = reduced - turns * 7.54978995489188216e-8
    square = reduced * reduced
    sine = ((-1.9515295891e-4 * square + 8.3321608736e-3) * square - 1.6666654611e-1) * square * reduced + reduced
    cosine = ((2.443315711809948e-5 * square - 1.388731625493765e-3) * square + 4.166664568298827e-2) * square * square - 0.5 * square + 1.0
    quadrant = turns.astype(jnp.int32)
    swap = (quadrant & 1) == 1
    out_sin = jnp.where(swap, cosine, sine)
    out_cos = jnp.where(swap, sine, cosine)
    out_sin = jnp.where((quadrant & 2) == 2, -out_sin, out_sin)
    out_cos = jnp.where(((quadrant + 1) & 2) == 2, -out_cos, out_cos)
    return out_sin, out_cos


def split_hi_lo(array):
    high = array.astype(jnp.bfloat16).astype(jnp.float32)
    return high, array - high


def geometry(points, observers, right_ref, cos_ref, sin_ref):
    offsets = [observers[i : i + 1, :] - points[:, i : i + 1] for i in range(3)]
    squared = offsets[0] * offsets[0] + offsets[1] * offsets[1] + offsets[2] * offsets[2]
    distance = jnp.sqrt(squared)
    inverse = 1.0 / distance
    weight = inverse * (1.0 / (4.0 * math.pi))
    far = [offset * (inverse * weight) for offset in offsets]
    near = [term * inverse for term in far]
    slots = near + far + [weight, jnp.zeros_like(weight)]
    high, low = split_hi_lo(jnp.concatenate(slots, axis=0))
    right_ref[...] = jnp.concatenate([high, low], axis=0).astype(jnp.bfloat16)
    sine, cosine = sin_cos(KAPPA * distance)
    twice = 2.0 * cosine
    past_cos, past_sin = jnp.ones_like(cosine), jnp.zeros_like(sine)
    for order in range(8):
        cos_ref[:, order, :] = cosine
        sin_ref[:, order, :] = sine
        cosine, past_cos = twice * cosine - past_cos, cosine
        sine, past_sin = twice * sine - past_sin, sine


def load_right(right_ref):
    half = right_ref.shape[0] // 2
    high, low = right_ref[:half, :], right_ref[half:, :]
    right = jnp.concatenate([high, high, low, low], axis=0)
    for unit in range(2):
        pltpu.matmul_push_rhs(right, staging_register=0, mxu_index=unit)


def amplitude(acc, y, left, fresh):
    lanes = lax.rem(lax.broadcasted_iota(jnp.int32, (1, left.shape[1]), 1), GROUP)
    one = left * (lanes == y).astype(jnp.float32).astype(jnp.bfloat16)
    both = jnp.concatenate([one, one], axis=1)
    pltpu.matmul_acc_lhs(acc, both, load_staged_rhs=0 if fresh else None)


def accumulate(amp, cosine, sine, step_cos, step_sin, acc_re, acc_im):
    blocks = len(acc_re)
    orders = amp.shape[0] // 2
    twice = 2.0 * step_cos
    past_cos = past_sin = None
    for b in range(blocks):
        amp_re = amp[8 * b : 8 * b + 8, :]
        amp_im = amp[orders + 8 * b : orders + 8 * b + 8, :]
        acc_re[b] = acc_re[b] + (amp_re * cosine + amp_im * sine)
        acc_im[b] = acc_im[b] + (amp_im * cosine - amp_re * sine)
        if b == 0:
            next_cos = cosine * step_cos - sine * step_sin
            next_sin = sine * step_cos + cosine * step_sin
        else:
            next_cos = twice * cosine - past_cos
            next_sin = twice * sine - past_sin
        past_cos, past_sin, cosine, sine = cosine, sine, next_cos, next_sin


def whole_kernel(
    share,
    flow_hbm,
    weight_ref,
    owner_ref,
    block_ref,
    normal_ref,
    point_ref,
    observer_ref,
    table_ref,
    out_ref,
    flow_ref,
    slices,
    flows,
    weights,
    facts,
    onehot,
    outgoing,
    series_ref,
    observers_ref,
    points,
    rights,
    cosines,
    sines,
    terms,
    shifted,
    lefts,
    acc_ref,
    sums,
    arrived,
    flow_send,
    flow_recv,
    weight_send,
    weight_recv,
    fact_send,
    fact_recv,
    view_send,
    view_recv,
    series_send,
    series_recv,
    term_send,
    term_recv,
    flow_load,
):
    owners = flows.shape[0]
    held = flow_ref.shape[0]
    cells = flow_ref.shape[1]
    spread = observers_ref.shape[0]
    members = share * spread
    samples = NT // members
    width = NV * samples
    slots = weight_ref.shape[1] // cells
    me_panel = lax.axis_index("panel")
    me_obs = lax.axis_index("obs")
    sub = lax.rem(me_panel, share)
    base = me_panel - sub
    mine = me_obs * share + sub

    def member(distance):
        return {
            "panel": base + flip(sub, distance // spread, share),
            "obs": flip(me_obs, distance % spread if isinstance(distance, int) else lax.rem(distance, spread), spread),
        }

    orders = acc_ref.shape[0] // 2
    panels = point_ref.shape[1]
    groups = panels // GROUP
    rows_out = out_ref.shape[1]
    ahead = onehot.shape[0] == members
    load = pltpu.make_async_copy(flow_hbm, flow_ref, flow_load)
    load.start()
    barrier = pltpu.get_barrier_semaphore()
    for turn in range(spread):

        def greet(shift, carry):
            pl.semaphore_signal(
                barrier,
                inc=1,
                device_id={"panel": lax.rem(me_panel + shift, owners), "obs": lax.rem(me_obs + turn, spread)},
                device_id_type=MESH,
            )
            return carry

        lax.fori_loop(1 if turn == 0 else 0, owners, greet, 0)

    def prepare(*accs):
        quarters, squares, talls, middles = accs[0:4], accs[4:6], accs[6:8], accs[8:10]
        facts[0] = jnp.zeros(facts.shape[1:], jnp.float32)
        facts[0, 0:1, :] = owner_ref[...].astype(jnp.float32)
        facts[0, 1:2, :] = block_ref[...].astype(jnp.float32)
        facts[0, 2:5, :] = normal_ref[...]
        place = lax.broadcasted_iota(jnp.int32, (slots * cells, slots * cells), 0)
        goal = lax.broadcasted_iota(jnp.int32, (slots * cells, slots * cells), 1)
        turn = hot(lax.rem(place, cells) * slots + place // cells == goal)
        for unit in range(2):
            span = slice(unit * 256, (unit + 1) * 256)
            tiles = [weight_ref[:, :256], weight_ref[:, 256:]]
            weights[0, :, span] = product(squares[unit], unit, tiles, [turn[:256, span], turn[256:, span]]).astype(jnp.bfloat16)
        observers_ref[me_obs] = observer_ref[...]

        points[...] = jnp.zeros_like(points)
        points[0:3, :] = point_ref[...]
        points[...] = jnp.transpose(points[...])

        pl.semaphore_wait(barrier, owners * spread - 1)

        def flow_copy(shift):
            target = flip(me_panel, shift, owners)
            return pltpu.make_async_remote_copy(
                src_ref=slices.at[lax.rem(target, share)],
                dst_ref=flows.at[me_panel],
                send_sem=flow_send.at[shift],
                recv_sem=flow_recv.at[shift],
                device_id={"panel": target},
                device_id_type=MESH,
            )

        def push(turn, carry):
            flow_copy(owners - turn).start()
            return carry

        def relay(buffer, send_sem, recv_sem, held_slot, bit):
            return pltpu.make_async_remote_copy(
                src_ref=buffer.at[held_slot],
                dst_ref=buffer.at[held_slot + bit],
                send_sem=send_sem.at[held_slot + bit],
                recv_sem=recv_sem.at[held_slot + bit],
                device_id=member(bit),
                device_id_type=MESH,
            )

        copies = {}

        def forward(slot):
            inner = slot % spread
            lowest = inner & -inner if inner else spread
            steps = [part * spread for part in range(1, share)] if slot == 0 else []
            bit = spread // 2
            while bit >= 1:
                steps.append(bit)
                bit //= 2
            for bit in steps:
                if bit < lowest or bit >= spread:
                    for kind, (buffer, send_sem, recv_sem) in enumerate(
                        ((facts, fact_send, fact_recv), (weights, weight_send, weight_recv))
                    ):
                        copy = relay(buffer, send_sem, recv_sem, slot, bit)
                        copy.start()
                        copies[kind, slot + bit] = copy

        forward(0)

        quarter = share * samples
        rows = lax.broadcasted_iota(jnp.int32, (2 * quarter, 256), 0)
        columns = lax.broadcasted_iota(jnp.int32, (2 * quarter, 256), 1)
        shift = lax.rem(me_obs * quarter, 128)
        tile = pl.multiple_of(me_obs * quarter - shift, 128)
        pick = hot((columns // 128 == rows // quarter) & (lax.rem(columns, 128) == lax.rem(rows, quarter) + shift))
        load.wait()
        for turn, (cell, var) in enumerate((cell, var) for cell in range(0, cells, 2) for var in range(0, NV, 2)):
            halves = [var, min(var + 1, NV - 1)]
            right = jnp.concatenate(
                [
                    jnp.concatenate([flow_ref[:, cell + side, pl.ds(one * NT + tile, 128)] for one in halves], axis=1)
                    for side in range(2)
                ],
                axis=0,
            )
            piece = product(quarters[turn % 4], turn % 2, [pick], [right], True).astype(jnp.bfloat16)
            for half in range(len(set(halves))):
                for side in range(2):
                    for part in range(share):
                        row = (cell + side) * width + (var + half) * samples
                        start = half * quarter + part * samples
                        slices[part, row : row + samples, :] = piece[
                            start : start + samples, side * held : (side + 1) * held
                        ]

        lax.fori_loop(1, owners, push, 0)

        def view_copy(shift):
            return pltpu.make_async_remote_copy(
                src_ref=observer_ref,
                dst_ref=observers_ref.at[me_obs],
                send_sem=view_send.at[shift],
                recv_sem=view_recv.at[shift],
                device_id={"obs": lax.rem(me_obs + shift, spread)},
                device_id_type=MESH,
            )

        views = [view_copy(shift) for shift in range(1, spread)]
        for view in views:
            view.start()
        flows[me_panel] = slices[sub]

        def survey(step):
            observers = observers_ref[lax.rem(me_obs + step + 1, spread)]

            @pl.loop(0, groups)
            def _(group):
                place = step * groups + group
                near = points[pl.ds(pl.multiple_of(group * GROUP, GROUP), GROUP), :]
                geometry(near, observers, rights.at[place], cosines.at[place], sines.at[place])

        def receive(slots_now):
            for slot in slots_now:
                copies[0, slot].wait_recv()
                copies[1, slot].wait_recv()
                forward(slot)

        order = sorted(
            range(1, members),
            key=lambda slot: (bin(slot % spread).count("1"), -(slot % spread), bin(slot).count("1"), -slot),
        )
        direct = share - 1
        survey(spread - 1)
        receive(order[:direct])
        for view in views:
            view.wait()
        for step in range(spread - 1):
            if step == 2:
                receive(order[direct : direct + share])
            survey(step)
        ends = order[direct + share :]
        for slot in ends:
            copies[0, slot].wait_recv()

        names = lax.broadcasted_iota(jnp.int32, (held, slots), 0).astype(jnp.float32)

        def mark(slot, side):
            owner_row = facts[slot, 0:1, :]
            block_row = facts[slot, 1:2, :]

            def mark_owner(owner, inner):
                row = jnp.where(owner_row == owner.astype(jnp.float32), block_row, -1.0)
                onehot[side, pl.ds(pl.multiple_of(owner * held, held), held), :] = hot(names == row)
                return inner

            lax.fori_loop(0, owners, mark_owner, 0)

        if ahead:

            @pl.loop(0, members)
            def _(slot):
                mark(slot, slot)

        def drain(shift, carry):
            flow_copy(shift).wait()
            return carry

        lax.fori_loop(1, owners, drain, 0)
        for slot in ends:
            copies[1, slot].wait_recv()

        chunk = min(owners, 8)

        def gathered(low, high):
            if not ahead:
                mark(low, 0)
                mark(high, 1)
            sides = (low, high) if ahead else (0, 1)

            def partial_of(start):
                terms_of = []
                for unit in range(2):
                    some = range(unit * chunk // 2, (unit + 1) * chunk // 2, 2)
                    left = [jnp.concatenate([flows[start + i], flows[start + i + 1]], axis=1) for i in some]
                    right = []
                    for i in some:
                        row = pl.ds(pl.multiple_of((start + i) * held, held), 2 * held)
                        right.append(jnp.concatenate([onehot[sides[0], row, :], onehot[sides[1], row, :]], axis=1))
                    terms_of.append(product(talls[unit], unit, left, right))
                return terms_of[0] + terms_of[1]

            total = partial_of(0)
            if owners > chunk:
                total = lax.fori_loop(1, owners // chunk, lambda i, run: run + partial_of(i * chunk), total)
            return total.astype(jnp.bfloat16)

        def values_of(low, high, donors):
            terms_of = []
            for unit in range(2):
                pairs = range(unit * cells // 2, (unit + 1) * cells // 2)
                left = []
                for side in range(2):
                    lanes = slice(side * slots, (side + 1) * slots)
                    left.append(jnp.concatenate([donors[cell * width : (cell + 1) * width, lanes] for cell in pairs], axis=1))
                span = slice(unit * 256, (unit + 1) * 256)
                right = jnp.concatenate([weights[low, :, span], weights[high, :, span]], axis=0)
                terms_of.append(product(middles[unit], unit, [jnp.concatenate(left, axis=0)], [right], True))
            both = terms_of[0] + terms_of[1]
            return both[:width, :panels], both[width:, panels:]

        def series_of(slot, values):
            field = [values[var * samples : (var + 1) * samples, :] for var in range(NV)]
            normal = [facts[slot, 2 + i : 3 + i, :] for i in range(3)]
            flow = field[1] * normal[0] + field[2] * normal[1] + field[3] * normal[2]
            mass = (1.0 + field[0]) * flow
            return [mass] + [field[4] * normal[i] + mass * field[1 + i] for i in range(3)]

        span = pl.ds(pl.multiple_of(mine * samples, samples), samples)

        def series_copy(slot):
            return pltpu.make_async_remote_copy(
                src_ref=outgoing.at[slot],
                dst_ref=series_ref.at[:, span, :],
                send_sem=series_send.at[slot],
                recv_sem=series_recv.at[slot],
                device_id=member(slot),
                device_id_type=MESH,
            )

        def finish(slot, values):
            for kind, term in enumerate(series_of(slot, values)):
                outgoing[slot, kind] = term
            series_copy(slot).start()


        def pair(step, donors):
            low = members - 2 * step
            high = low + 1
            following = gathered(low - 2, high - 2)
            first_values, second_values = values_of(low, high, donors)
            finish(low, first_values)
            finish(high, second_values)
            return following

        donors = lax.fori_loop(1, members // 2, pair, gathered(members - 2, members - 1))
        low_values, high_values = values_of(0, 1, donors)
        finish(1, high_values)
        for kind, term in enumerate(series_of(0, low_values)):
            series_ref[kind, span, :] = term

        for slot in range(1, members):
            copies[0, slot].wait_send()
            copies[1, slot].wait_send()

        def settle_series(slot, carry):
            series_copy(slot).wait()
            return carry

        lax.fori_loop(1, members, settle_series, 0)

        wavenum = KAPPA * (1 + lax.broadcasted_iota(jnp.int32, (orders, panels), 0)).astype(jnp.float32)
        for unit in range(2):
            rest = jnp.concatenate([series_ref[2 * unit], series_ref[2 * unit + 1]], axis=1)
            left, right = [], []
            for depth in range(3):
                part = rest.astype(jnp.bfloat16)
                rest = rest - part.astype(jnp.float32)
                for level in range(3 - depth):
                    left.append(table_ref[level])
                    right.append(part)
            both = product(squares[unit], unit, left, right)
            for side in range(2):
                kind = 2 * unit + side
                near = both[:, side * panels : (side + 1) * panels]
                far = jnp.concatenate([-wavenum * near[orders:], wavenum * near[:orders]], axis=0)
                if kind == 0:
                    terms[6] = far
                else:
                    terms[kind - 1] = near
                    terms[kind + 2] = far
        lane = lax.broadcasted_iota(jnp.int32, (1, panels), 1)

        for slot in range(SLOT - 1):
            high, low = split_hi_lo(terms[slot])
            shifted[slot] = pltpu.roll(high, slot * GROUP, 1) if slot else high
            shifted[SLOT + slot] = pltpu.roll(low, (SLOT + slot) * GROUP, 1)

        @pl.loop(0, groups)
        def _(group):
            kind = lax.rem(lane // GROUP + (groups - group), groups)
            both = jnp.zeros((2 * orders, panels), jnp.float32)
            for slot in range(SLOT - 1):
                both = jnp.where(kind == slot, shifted[slot], both)
                both = jnp.where(kind == SLOT + slot, shifted[SLOT + slot], both)
            moved = pltpu.roll(both, lax.rem((groups - group) * GROUP, panels), 1)
            lefts[group] = moved.astype(jnp.bfloat16)

    def term_copy(step, shift):
        slot = lax.rem(step + 1, spread) * owners + shift
        target = lax.rem(me_panel + shift, owners)
        return pltpu.make_async_remote_copy(
            src_ref=sums.at[step, target],
            dst_ref=arrived.at[slot],
            send_sem=term_send.at[slot],
            recv_sem=term_recv.at[slot],
            device_id={"panel": target, "obs": lax.rem(me_obs + step + 1, spread)},
            device_id_type=MESH,
        )

    def radiate(*accs):

        last = spread * groups - 1
        load_right(rights.at[0])
        for y in range(GROUP):
            amplitude(accs[y], y, lefts[0], y < 2)
        load_right(rights.at[1])

        @pl.loop(0, spread)
        def _(step):
            acc_ref[...] = jnp.zeros_like(acc_ref)

            @pl.loop(0, groups)
            def _(group):
                place = step * groups + group
                after = jnp.minimum(place + 1, last)
                left = lefts[lax.rem(after, groups)]
                blocks = orders // 8
                acc_re = [acc_ref[pl.ds(8 * b, 8), :] for b in range(blocks)]
                acc_im = [acc_ref[pl.ds(orders + 8 * b, 8), :] for b in range(blocks)]
                for y in range(GROUP):
                    amp = pltpu.matmul_pop(accs[y])
                    amplitude(accs[y], y, left, y < 2)
                    if y == 1:
                        load_right(rights.at[jnp.minimum(place + 2, last)])
                    steps = (cosines[place, y, 7:8, :], sines[place, y, 7:8, :])
                    accumulate(amp, cosines[place, y], sines[place, y], *steps, acc_re, acc_im)
                for b in range(blocks):
                    acc_ref[pl.ds(8 * b, 8), :] = acc_re[b]
                    acc_ref[pl.ds(orders + 8 * b, 8), :] = acc_im[b]

            for owner in range(owners):
                sums[step, owner] = acc_ref[owner * rows_out : (owner + 1) * rows_out, :]

            @pl.when(step < spread - 1)
            def _():
                term_copy(step, 0).start()

            def push(shift, carry):
                term_copy(step, shift).start()
                return carry

            lax.fori_loop(1, owners, push, 0)

        for y in range(2):
            amplitude(accs[y], y, lefts[0], True)
        for acc in accs:
            pltpu.matmul_pop(acc)

    def store(unit, height):
        return pltpu.ACC(unit)((height, 256), jnp.float32)

    part_rows = share * samples
    pl.run_scoped(
        prepare,
        *[store(turn % 2, 2 * part_rows) for turn in range(4)],
        *[store(unit, 2 * orders) for unit in range(2)],
        *[store(unit, cells * width) for unit in range(2)],
        *[store(unit, 2 * width) for unit in range(2)],
    )
    pl.run_scoped(radiate, *[store(y % 2, 2 * orders) for y in range(GROUP)])

    def settle(step):
        def one(shift, carry):
            term_copy(step, shift).wait()
            return carry

        lax.fori_loop(1 if step == spread - 1 else 0, owners, one, 0)

    def add(slot, total):
        return total + arrived[slot]

    for step in range(spread - 1):
        settle(step)
    early = lax.fori_loop(owners, owners * spread, add, sums[spread - 1, me_panel])
    out_ref[0] = early
    settle(spread - 1)
    out_ref[1] = lax.fori_loop(2, owners, add, arrived[1])


def run(flow, weight, owner, block, normals, points, observers):
    owners = lax.axis_size("panel")
    spread = lax.axis_size("obs")
    share = max(1, min(owners, 16 // spread))
    members = share * spread
    held, cells, history = flow.shape
    panels = normals.shape[1]
    count = observers.shape[1]
    samples = NT // members
    width = NV * samples
    slots = weight.shape[1] // cells
    places = spread * (panels // GROUP)
    rows = 2 * HARM // owners
    ahead = members * owners * held * slots <= 1 << 22
    bf16, f32 = jnp.bfloat16, jnp.float32
    vmem = pl.BlockSpec(memory_space=pltpu.VMEM)
    dma = pltpu.SemaphoreType.DMA
    wave = pltpu.VMEM((places, GROUP, 8, count), f32)
    return pl.pallas_call(
        functools.partial(whole_kernel, share),
        out_shape=jax.ShapeDtypeStruct((2, rows, count), f32),
        in_specs=[pl.BlockSpec(memory_space=pl.ANY)] + [vmem] * 7,
        out_specs=vmem,
        scratch_shapes=[
            pltpu.VMEM(flow.shape, bf16),
            pltpu.VMEM((share, cells * width, held), bf16),
            pltpu.VMEM((owners, cells * width, held), bf16),
            pltpu.VMEM((members,) + weight.shape, bf16),
            pltpu.VMEM((members, 8, panels), f32),
            pltpu.VMEM((members if ahead else 2, owners * held, slots), bf16),
            pltpu.VMEM((members, SERIES, samples, panels), f32),
            pltpu.VMEM((SERIES, NT, panels), f32),
            pltpu.VMEM((spread,) + observers.shape, f32),
            pltpu.VMEM((panels, panels), f32),
            pltpu.VMEM((places, 2 * SLOT * GROUP, count), bf16),
            wave,
            wave,
            pltpu.VMEM((SLOT - 1, 2 * HARM, panels), f32),
            pltpu.VMEM((2 * SLOT, 2 * HARM, panels), f32),
            pltpu.VMEM((panels // GROUP, 2 * HARM, panels), bf16),
            pltpu.VMEM((2 * HARM, count), f32),
            pltpu.VMEM((spread, owners, rows, count), f32),
            pltpu.VMEM((spread * owners, rows, count), f32),
            dma((owners,)),
            dma((owners,)),
            dma((members,)),
            dma((members,)),
            dma((members,)),
            dma((members,)),
            dma((spread,)),
            dma((spread,)),
            dma((members,)),
            dma((members,)),
            dma((spread * owners,)),
            dma((spread * owners,)),
            dma,
        ],
        compiler_params=pltpu.CompilerParams(
            collective_id=1,
            has_side_effects=True,
            vmem_limit_bytes=63000 * 1024,
        ),
        name="whole",
    )(flow, weight, owner, block, normals, points, observers, jnp.asarray(three_parts(fourier_rows(NT, HARM))))


def body(
    flow_blocks,
    interp_weights,
    donor_owner,
    donor_block,
    panel_normals,
    panel_points,
    observer_points,
):
    tiles, width, stencil = interp_weights.shape
    halves = run(
        flow_blocks,
        interp_weights.reshape(tiles * width, stencil),
        donor_owner.reshape(1, -1),
        donor_block.reshape(1, -1),
        panel_normals,
        panel_points,
        observer_points,
    )
    return halves[0] + halves[1]


def solution(mesh):
    return jax.shard_map(
        body,
        mesh=mesh,
        in_specs=(
            P("panel", None, None),
            P(("panel", "obs"), None, None),
            P(("panel", "obs"), None),
            P(("panel", "obs")),
            P(None, ("panel", "obs")),
            P(None, ("panel", "obs")),
            P(None, "obs"),
        ),
        out_specs=P("panel", "obs"),
        check_vma=False,
    )
```
